32 devices in a mesh: dp: 4 (over y, z), ep: 8 (over x, core).
Axes of the slice: x: 4, y: 2, z: 2, core: 2. Of those that a mesh axis runs over, the one named last changes fastest.
The devices are a block of a 4x4x8 slice.
Arguments:
- tokens: bfloat16 [6144, 2048], P(('dp', 'ep')), parts along dimension 0
- topk_idx: int32 [6144, 6], P(('dp', 'ep')), parts along dimension 0
- topk_w: float32 [6144, 6], P(('dp', 'ep')), parts along dimension 0
- w_up: bfloat16 [8, 9, 2048, 1408], P('ep')
- w_down: bfloat16 [8, 9, 1408, 2048], P('ep')
- slot_expert: int32 [8, 9], replicated
Outputs:
- output: bfloat16 [6144, 2048], P(('dp', 'ep')), parts along dimension 0
There are 4 independent parts. The reference program is written for one: setup_inputs(seed, part) draws one part's arguments, and reference() takes and returns one part's arrays. A program takes and returns all parts, laid end to end along the dimension named above; an argument that names none is the same for every part.
All inputs are finite; a program needn't handle non-finite values.
Results may differ from the reference program's by a relative error of at most 0.00137.
Values are sent between devices in bfloat16 or wider.
A program may use at most 768 MiB of HBM per device.

```python
import jax
import jax.numpy as jnp
from jax import lax
import numpy as np

GROUP = 8
TOK_DEV = 192
D_MODEL = 2048
D_FF = 1408
EXPERTS = 64
TOP = 6

PER_DEV = EXPERTS // GROUP
SLOTS = PER_DEV + 1
N_UNITS = GROUP * SLOTS
PAIRS_DEV = TOK_DEV * TOP
BASE_LOAD = PAIRS_DEV // N_UNITS
BLOCK = max(8, (GROUP * PAIRS_DEV) // N_UNITS)
N_BLOCKS = (GROUP * PAIRS_DEV) // BLOCK + EXPERTS


def base_table():
    dev_ids = np.arange(GROUP)
    hot_dev = (3 * (dev_ids // 3) + 3) % GROUP
    spare_exp = hot_dev * PER_DEV + PER_DEV - 1
    primary = np.arange(EXPERTS).reshape(GROUP, PER_DEV)
    return np.concatenate([primary, spare_exp[:, None]], axis=1).astype(np.int32)


def draw_table(key_tab):
    key_dev, key_col, key_lab = jax.random.split(key_tab, 3)
    relabel = jax.random.permutation(key_lab, EXPERTS).astype(jnp.int32)
    dev_perm = jax.random.permutation(key_dev, GROUP)
    col_perm = jax.random.permutation(key_col, SLOTS)
    slot_table = jnp.asarray(base_table())[dev_perm][:, col_perm]
    return relabel[slot_table], relabel


def draw_loads(key_load):
    key_perm, key_shift = jax.random.split(key_load)
    unit_order = 1 + jax.random.permutation(key_perm, N_UNITS - 1)
    shift_amt = jax.random.randint(key_shift, ((N_UNITS - 2) // 2,), 0, BASE_LOAD // 2 + 1, dtype=jnp.int32)
    spread = BASE_LOAD // 2 + 1
    unit_loads = jnp.full((N_UNITS,), BASE_LOAD, jnp.int32)
    unit_loads = unit_loads.at[0].add(spread).at[unit_order[0]].add(-spread)
    unit_loads = unit_loads.at[unit_order[1::2]].add(shift_amt).at[unit_order[2::2]].add(-shift_amt)
    return unit_loads.at[unit_order[:PAIRS_DEV - N_UNITS * BASE_LOAD]].add(1)


def draw_routing(key_src, unit_expert):
    key_load, key_tok = jax.random.split(key_src)
    counts = jax.ops.segment_sum(draw_loads(key_load), unit_expert, num_segments=EXPERTS)
    bounds = jnp.cumsum(counts)
    sorted_exp = jnp.searchsorted(bounds, jnp.arange(PAIRS_DEV, dtype=jnp.int32), side='right').astype(jnp.int32)
    routes = sorted_exp.reshape(TOP, TOK_DEV).T
    return routes[jax.random.permutation(key_tok, TOK_DEV)]


def setup_inputs(seed: int = 0, part: int = 0) -> dict:
    root_key = jax.random.key(seed)
    key_tab, key_up, key_down, key_part = jax.random.split(root_key, 4)
    slot_expert, relabel = draw_table(key_tab)
    unit_expert = relabel[jnp.asarray(base_table()).reshape(-1)]
    up_base = jax.random.normal(key_up, (EXPERTS, D_MODEL, D_FF), jnp.float32) * D_MODEL ** -0.5
    down_base = jax.random.normal(key_down, (EXPERTS, D_FF, D_MODEL), jnp.float32) * D_FF ** -0.5
    key_grp = jax.random.fold_in(key_part, part)
    key_tokens, key_gate, key_route = jax.random.split(key_grp, 3)
    tokens = jax.random.normal(key_tokens, (GROUP * TOK_DEV, D_MODEL), jnp.float32)
    topk_w = jax.random.uniform(key_gate, (GROUP * TOK_DEV, TOP), jnp.float32, 0.3, 1.0)
    src_keys = jax.random.split(key_route, GROUP)
    topk_idx = jax.vmap(draw_routing, in_axes=(0, None))(src_keys, unit_expert)
    return {'tokens': tokens.astype(jnp.bfloat16), 'topk_idx': topk_idx.reshape(GROUP * TOK_DEV, TOP), 'topk_w': topk_w, 'w_up': up_base.astype(jnp.bfloat16)[slot_expert], 'w_down': down_base.astype(jnp.bfloat16)[slot_expert], 'slot_expert': slot_expert}


def reference(tokens, topk_idx, topk_w, w_up, w_down, slot_expert):
    n_tok = tokens.shape[0]
    n_pairs = n_tok * TOP
    table_flat = slot_expert.reshape(-1)
    first_slot = jax.ops.segment_min(jnp.arange(N_UNITS, dtype=jnp.int32), table_flat, num_segments=EXPERTS)
    up_flat = w_up.reshape(N_UNITS, D_MODEL, D_FF)
    down_flat = w_down.reshape(N_UNITS, D_FF, D_MODEL)
    flat_exp = topk_idx.reshape(-1)
    flat_gate = topk_w.reshape(-1)
    pair_order = jnp.argsort(flat_exp, stable=True)
    counts = jnp.bincount(flat_exp, length=EXPERTS)
    starts = jnp.cumsum(counts) - counts
    exp_blocks = (counts + BLOCK - 1) // BLOCK
    block_end = jnp.cumsum(exp_blocks)
    block_start = block_end - exp_blocks
    lane_ids = jnp.arange(BLOCK)

    def block_step(acc_sum, block_id):
        exp_id = jnp.minimum(jnp.searchsorted(block_end, block_id, side='right'), EXPERTS - 1)
        offsets = (block_id - block_start[exp_id]) * BLOCK + lane_ids
        is_valid = (offsets < counts[exp_id]) & (block_id < block_end[EXPERTS - 1])
        pair_ids = pair_order[jnp.clip(starts[exp_id] + offsets, 0, n_pairs - 1)]
        tok_ids = pair_ids // TOP
        slot_id = first_slot[exp_id]
        pre_act = jnp.dot(tokens[tok_ids], up_flat[slot_id], preferred_element_type=jnp.float32)
        hidden = jax.nn.gelu(pre_act, approximate=True).astype(jnp.bfloat16)
        expert_out = jnp.dot(hidden, down_flat[slot_id], preferred_element_type=jnp.float32).astype(jnp.bfloat16)
        gate_vals = jnp.where(is_valid, flat_gate[pair_ids], 0.0)
        return acc_sum.at[tok_ids].add(gate_vals[:, None] * expert_out.astype(jnp.float32)), None

    acc_out, _ = lax.scan(block_step, jnp.zeros((n_tok, D_MODEL), jnp.float32), jnp.arange(N_BLOCKS))
    return acc_out.astype(jnp.bfloat16)
```

```python
import functools

import jax
import jax.numpy as jnp
from jax import lax
from jax.experimental import pallas as pl
from jax.experimental.pallas import tpu as pltpu
from jax.sharding import PartitionSpec as P

MESH = pl.DeviceIdType.MESH
F32 = jnp.float32
BF16 = jnp.bfloat16
LANES = 128
CHIPS = 4
AHEAD = 2
STAGES = 4


def slot_bound(n_tok, n_top, n_dev, n_slot):
    base_load = (n_tok * n_top) // (n_dev * n_slot)
    return base_load + base_load // 2 + 1


def round_up(n, m):
    return -(-n // m) * m


def gelu(v):
    return v * (0.5 + 0.5 * jnp.tanh(v * (0.7978845608028654 + (0.7978845608028654 * 0.044715) * (v * v))))


def dot(a, b):
    return lax.dot_general(a, b, (((1,), (0,)), ((), ())), preferred_element_type=F32)


def moe_kernel(cfg, x_ref, meta_ref, ecol_ref, trk_ref, wup_ref, wdn_ref, y_ref,
               xall, meta_all, g_buf, c_buf, xg, acc, h_buf, o_buf, wu, wd, sib_in, far_in, dir_in, mrg_in,
               meta_ss, meta_rs, near_ss, near_rs, rel_ss, rel_rs, sib_ss, sib_rs, wu_s, wd_s,
               ps_ss, ps_rs, pf_ss, pf_rs, pd_ss, pd_rs, pm_ss, pm_rs):
    n_tok, d_model, d_ff, n_slot, cap, kb_w, cb_w, n_top, d_mid = (
        cfg[k] for k in ("n_tok", "d_model", "d_ff", "n_slot", "cap", "kb_w", "cb_w", "n_top", "d_mid"))
    n_kb, n_cb = d_model // kb_w, d_model // cb_w
    n_src = 2 * CHIPS
    half = n_tok // 2
    nu, nd = wu.shape[0], wd.shape[0]
    me = lax.axis_index("ep")
    chip, core = me // 2, me % 2

    def dev(d_chip, d_core=0):
        return {"ep": ((chip + d_chip) % CHIPS) * 2 + (core + d_core) % 2}

    right, left, sib = dev(1), dev(CHIPS - 1), dev(0, 1)

    def rcopy(src, dst, ss, rs, to):
        return pltpu.make_async_remote_copy(src_ref=src, dst_ref=dst, send_sem=ss, recv_sem=rs, device_id=to, device_id_type=MESH)

    def up_load(i):
        return pltpu.make_async_copy(
            wup_ref.at[0, i % n_slot, pl.ds(pl.multiple_of((i // n_slot) * kb_w, kb_w), kb_w), :], wu.at[i % nu], wu_s.at[i % nu])

    def down_load(i):
        return pltpu.make_async_copy(
            wdn_ref.at[0, i % n_slot, :, pl.ds(pl.multiple_of((i // n_slot) * cb_w, cb_w), cb_w)], wd.at[i % nd], wd_s.at[i % nd])

    for i in range(nu):
        up_load(i).start()

    barrier = pltpu.get_barrier_semaphore()
    peers = [(dx, dc) for dx in range(CHIPS) for dc in range(2) if dx or dc]
    for dx, dc in peers:
        pl.semaphore_signal(barrier, inc=1, device_id=dev(dx, dc), device_id_type=MESH)
    pl.semaphore_wait(barrier, len(peers))

    sends = []

    def go(copy):
        copy.start()
        sends.append(copy)

    def own(kb):
        return x_ref.at[:, pl.ds(kb * kb_w, kb_w)]

    near = [(rcopy(own(kb), xall.at[2 * (CHIPS - 1), kb], near_ss.at[kb, 0], near_rs.at[kb, 0], right),
             rcopy(own(kb), xall.at[2, kb], near_ss.at[kb, 1], near_rs.at[kb, 1], left)) for kb in range(n_kb)]
    lo, hi = pl.ds(0, half), pl.ds(half, n_tok - half)
    relay = [(rcopy(xall.at[2 * (CHIPS - 1), kb, lo], xall.at[4, kb, lo], rel_ss.at[kb, 0], rel_rs.at[kb, 0], right),
              rcopy(xall.at[2, kb, hi], xall.at[4, kb, hi], rel_ss.at[kb, 1], rel_rs.at[kb, 1], left)) for kb in range(n_kb)]
    across = [[rcopy(own(kb) if off == 0 else xall.at[2 * off, kb], xall.at[2 * off + 1, kb],
                     sib_ss.at[kb, off], sib_rs.at[kb, off], sib) for off in range(CHIPS)] for kb in range(n_kb)]
    metas = []
    for n, (dx, dc) in enumerate(peers):
        metas.append(rcopy(meta_ref, meta_all.at[2 * ((CHIPS - dx) % CHIPS) + dc], meta_ss.at[n], meta_rs.at[n], dev(dx, dc)))

    for m in metas:
        go(m)
    for kb in range(min(AHEAD, n_kb)):
        go(near[kb][0])
        go(near[kb][1])
    for kb in range(n_kb):
        go(across[kb][0])

    meta_all[0] = meta_ref[...]
    for kb in range(n_kb):
        xall[0, kb] = x_ref[:, kb * kb_w:(kb + 1) * kb_w]

    def stage_near(kb):
        for c, r, off in ((near[kb][0], relay[kb][0], CHIPS - 1), (near[kb][1], relay[kb][1], 1)):
            c.wait_recv()
            go(r)
            go(across[kb][off])
        if kb + AHEAD < n_kb:
            go(near[kb + AHEAD][0])
            go(near[kb + AHEAD][1])

    for m in metas:
        m.wait_recv()
    lane_tok = meta_ref.shape[1]
    earlier = (lax.broadcasted_iota(jnp.int32, (lane_tok, lane_tok), 0)
               < lax.broadcasted_iota(jnp.int32, (lane_tok, lane_tok), 1)).astype(F32).astype(BF16)
    e_col = ecol_ref[:, 0:1]
    rows_src = n_slot * cap
    rows_pad = round_up(rows_src, LANES)

    def route(j, carry):
        m = meta_all[j]
        has = jnp.zeros((ecol_ref.shape[0], lane_tok), F32)
        gate = jnp.zeros((ecol_ref.shape[0], lane_tok), F32)
        for q in range(n_top):
            hit = m[q:q + 1, :] == e_col
            has = jnp.where(hit, 1.0, has)
            gate = jnp.where(hit, m[8 + q:9 + q, :], gate)
        rank = jnp.where(has > 0.0, dot(has.astype(BF16), earlier), -1.0)
        parts = []
        for s in range(n_slot):
            hit = rank[s:s + 1, :] == trk_ref[s * cap:(s + 1) * cap, 0:1]
            g_buf[j, s * cap:(s + 1) * cap, :] = jnp.where(hit, 1.0, 0.0)[:, :n_tok].astype(BF16)
            parts.append(jnp.where(hit, gate[s:s + 1, :], 0.0))
        if rows_pad > rows_src:
            parts.append(jnp.zeros((rows_pad - rows_src, lane_tok), F32))
        gates = jnp.transpose(jnp.concatenate(parts, axis=0))[:n_tok, :rows_src]
        for n in range(3):
            term = gates.astype(BF16)
            c_buf[j, n * n_tok:(n + 1) * n_tok, :] = term
            gates = gates - term.astype(F32)
        return carry

    lax.fori_loop(0, n_src, route, 0)

    chunks = [(n, min(2 * LANES, d_ff - n)) for n in range(0, d_ff, 2 * LANES)]
    n_mid = d_ff // LANES

    stage_near(0)
    for kb in range(n_kb):
        if kb + 1 < n_kb:
            stage_near(kb + 1)
        relay[kb][0].wait_recv()
        relay[kb][1].wait_recv()
        go(across[kb][2])
        for c in across[kb]:
            c.wait_recv()

        def gather(j, carry, kb=kb):
            rows = dot(g_buf[j], xall[j, kb]).astype(BF16)
            for s in range(n_slot):
                xg[s, pl.ds(pl.multiple_of(j * cap, cap), cap), :] = rows[s * cap:(s + 1) * cap]
            return carry

        lax.fori_loop(0, n_src, gather, 0)

        def up(s, carry, kb=kb):
            i = kb * n_slot + s
            up_load(i).wait()
            for n0, nw in chunks:
                v = dot(xg[s], wu[i % nu, :, n0:n0 + nw])
                for n in range(0, nw, LANES):
                    q = s * n_mid + (n0 + n) // LANES
                    part = v[:, n:n + LANES]
                    if kb > 0:
                        part = acc[q, :d_mid, :] + part
                    if kb < n_kb - 1:
                        acc[q, :d_mid, :] = part
                    else:
                        h_buf[s, :, n0 + n:n0 + n + LANES] = gelu(part).astype(BF16)

            @pl.when(i + nu < n_kb * n_slot)
            def _():
                up_load(i + nu).start()
            return carry

        lax.fori_loop(0, n_slot, up, 0)
        if kb == 0:
            for i in range(nd):
                down_load(i).start()

    def mine(cb, off, h):
        return (cb * CHIPS + off) * 2 + h

    def staged(cb, off, h):
        return n_cb * CHIPS * 2 + ((cb % STAGES) * CHIPS + off) * 2 + h

    tok = pl.ds(0, n_tok)
    to_sib = [[rcopy(acc.at[pl.ds(staged(cb, off, 0), 2), tok], sib_in.at[cb, off], ps_ss.at[cb, off], ps_rs.at[cb, off], sib)
               for off in range(CHIPS)] for cb in range(n_cb)]
    to_far = [(rcopy(acc.at[mine(cb, 2, 0), tok], far_in.at[cb, 0], pf_ss.at[cb, 0], pf_rs.at[cb, 0], right),
               rcopy(acc.at[mine(cb, 2, 1), tok], far_in.at[cb, 1], pf_ss.at[cb, 1], pf_rs.at[cb, 1], left)) for cb in range(n_cb)]
    to_dir = [(rcopy(acc.at[mine(cb, 1, 1), tok], dir_in.at[cb, 0], pd_ss.at[cb, 0], pd_rs.at[cb, 0], right),
               rcopy(acc.at[mine(cb, 3, 0), tok], dir_in.at[cb, 1], pd_ss.at[cb, 1], pd_rs.at[cb, 1], left)) for cb in range(n_cb)]
    to_mrg = [(rcopy(far_in.at[cb, 0], mrg_in.at[cb, 0], pm_ss.at[cb, 0], pm_rs.at[cb, 0], right),
               rcopy(far_in.at[cb, 1], mrg_in.at[cb, 1], pm_ss.at[cb, 1], pm_rs.at[cb, 1], left)) for cb in range(n_cb)]
    waited = set()

    def merge(cb):
        to_far[cb][0].wait_recv()
        far_in[cb, 0] = far_in[cb, 0] + acc[mine(cb, 1, 0), :n_tok, :]
        go(to_mrg[cb][0])
        to_far[cb][1].wait_recv()
        far_in[cb, 1] = far_in[cb, 1] + acc[mine(cb, 3, 1), :n_tok, :]
        go(to_mrg[cb][1])

    def finish(cb):
        for h in range(2):
            to_mrg[cb][h].wait_recv()
            to_dir[cb][1 - h].wait_recv()
            total = acc[mine(cb, 0, h), :n_tok, :] + mrg_in[cb, h] + dir_in[cb, 1 - h]
            y_ref[:, cb * cb_w + h * LANES:cb * cb_w + (h + 1) * LANES] = total.astype(BF16)

    for cb in range(n_cb):
        def down(s, carry, cb=cb):
            i = cb * n_slot + s
            down_load(i).wait()
            out = dot(h_buf[s], wd[i % nd]).astype(BF16)
            for j in range(n_src):
                o_buf[j, pl.ds(pl.multiple_of(s * cap, cap), cap), :] = out[j * cap:(j + 1) * cap]

            @pl.when(i + nd < n_cb * n_slot)
            def _():
                down_load(i + nd).start()
            return carry

        lax.fori_loop(0, n_slot, down, 0)
        if cb >= STAGES:
            for off in range(CHIPS):
                to_sib[cb - STAGES][off].wait_send()
                waited.add(id(to_sib[cb - STAGES][off]))

        def combine(off, carry, dc, first):
            v = dot(c_buf[2 * off + dc], o_buf[2 * off + dc])
            v = (v[2 * n_tok:] + v[n_tok:2 * n_tok]) + v[:n_tok]
            acc[first + 2 * off, :n_tok, :] = v[:, :LANES]
            acc[first + 2 * off + 1, :n_tok, :] = v[:, LANES:]
            return carry

        lax.fori_loop(0, CHIPS, functools.partial(combine, dc=1, first=staged(cb, 0, 0)), 0)
        for off in (2, 1, 3, 0):
            go(to_sib[cb][off])
        lax.fori_loop(0, CHIPS, functools.partial(combine, dc=0, first=mine(cb, 0, 0)), 0)
        for off in (2, 1, 3, 0):
            to_sib[cb][off].wait_recv()
            for h in range(2):
                q = mine(cb, off, h)
                acc[q, :n_tok, :] = acc[q, :n_tok, :] + sib_in[cb, off, h]
            if off == 2:
                go(to_far[cb][0])
                go(to_far[cb][1])
            elif off:
                go(to_dir[cb][0 if off == 1 else 1])
        if cb >= 1:
            merge(cb - 1)
        if cb >= 2:
            finish(cb - 2)
    merge(n_cb - 1)
    for cb in range(max(0, n_cb - 2), n_cb):
        finish(cb)
    for c in sends:
        if id(c) not in waited:
            c.wait_send()


def solution(mesh):
    assert mesh.shape["ep"] == 2 * CHIPS

    def group_layer(tokens, topk_idx, topk_w, w_up, w_down, slot_expert):
        n_tok, d_model = tokens.shape
        n_top = topk_idx.shape[1]
        n_dev, n_slot = slot_expert.shape
        d_ff = w_up.shape[-1]
        bound = slot_bound(n_tok, n_top, n_dev, n_slot)
        cap = round_up(bound, 16)
        kb_w, cb_w = 2 * LANES, 2 * LANES
        n_kb, n_cb = d_model // kb_w, d_model // cb_w
        n_src = n_dev
        lane_tok = round_up(n_tok, LANES)

        me = lax.axis_index("ep")
        flat = slot_expert.reshape(-1)
        n_all = flat.shape[0]
        same = flat[:, None] == flat[None, :]
        ids = jnp.arange(n_all, dtype=jnp.int32)
        copy_rank = jnp.sum(same & (ids[None, :] < ids[:, None]), axis=1, dtype=jnp.int32)
        copies = jnp.sum(same, axis=1, dtype=jnp.int32)
        my_exp = lax.dynamic_slice_in_dim(flat, me * n_slot, n_slot)
        my_rank = lax.dynamic_slice_in_dim(copy_rank, me * n_slot, n_slot)
        my_copies = lax.dynamic_slice_in_dim(copies, me * n_slot, n_slot)
        r = jnp.arange(cap, dtype=jnp.int32)[None, :]
        trk = jnp.where(r < bound, r * my_copies[:, None] + my_rank[:, None], -2).astype(F32).reshape(-1, 1)
        trk = jnp.broadcast_to(trk, (n_slot * cap, LANES))
        ecol = jnp.pad(my_exp.astype(F32), (0, round_up(n_slot, 8) - n_slot), constant_values=-2.0)
        ecol = jnp.broadcast_to(ecol[:, None], (ecol.shape[0], LANES))
        pad = ((0, 8 - n_top), (0, lane_tok - n_tok))
        meta = jnp.concatenate([jnp.pad(topk_idx.astype(F32).T, pad, constant_values=-1.0), jnp.pad(topk_w.T, pad)], axis=0)

        d_mid = n_src * cap
        n_mid = d_ff // LANES
        rows_src = n_slot * cap
        n_acc = max(n_slot * n_mid, (n_cb + STAGES) * CHIPS * 2)
        nu, nd = 6, 16
        cfg = dict(n_tok=n_tok, d_model=d_model, d_ff=d_ff, n_slot=n_slot, cap=cap, kb_w=kb_w, cb_w=cb_w, n_top=n_top, d_mid=d_mid)
        dma = pltpu.SemaphoreType.DMA
        vmem = pl.BlockSpec(memory_space=pltpu.VMEM)
        hbm = pl.BlockSpec(memory_space=pl.ANY)
        return pl.pallas_call(
            functools.partial(moe_kernel, cfg),
            out_shape=jax.ShapeDtypeStruct((n_tok, d_model), BF16),
            in_specs=[vmem, vmem, vmem, vmem, hbm, hbm],
            out_specs=vmem,
            scratch_shapes=[
                pltpu.VMEM((n_src, n_kb, n_tok, kb_w), BF16),
                pltpu.VMEM((n_src,) + meta.shape, F32),
                pltpu.VMEM((n_src, rows_src, n_tok), BF16),
                pltpu.VMEM((n_src, 3 * n_tok, rows_src), BF16),
                pltpu.VMEM((n_slot, d_mid, kb_w), BF16),
                pltpu.VMEM((n_acc, max(d_mid, n_tok), LANES), F32),
                pltpu.VMEM((n_slot, d_mid, d_ff), BF16),
                pltpu.VMEM((n_src, rows_src, cb_w), BF16),
                pltpu.VMEM((nu, kb_w, d_ff), BF16),
                pltpu.VMEM((nd, d_ff, cb_w), BF16),
                pltpu.VMEM((n_cb, CHIPS, 2, n_tok, LANES), F32),
                pltpu.VMEM((n_cb, 2, n_tok, LANES), F32),
                pltpu.VMEM((n_cb, 2, n_tok, LANES), F32),
                pltpu.VMEM((n_cb, 2, n_tok, LANES), F32),
                dma((n_src - 1,)), dma((n_src - 1,)),
                dma((n_kb, 2)), dma((n_kb, 2)), dma((n_kb, 2)), dma((n_kb, 2)),
                dma((n_kb, CHIPS)), dma((n_kb, CHIPS)),
                dma((nu,)), dma((nd,)),
                dma((n_cb, CHIPS)), dma((n_cb, CHIPS)),
                dma((n_cb, 2)), dma((n_cb, 2)), dma((n_cb, 2)), dma((n_cb, 2)), dma((n_cb, 2)), dma((n_cb, 2)),
            ],
            compiler_params=pltpu.CompilerParams(collective_id=0, has_side_effects=True, vmem_limit_bytes=67_000_000),
        )(tokens, meta, ecol, trk, w_up, w_down)

    row_spec = P(('dp', 'ep'), None)
    weight_spec = P('ep', None, None, None)
    return jax.shard_map(group_layer, mesh=mesh, in_specs=(row_spec, row_spec, row_spec, weight_spec, weight_spec, P(None, None)),
                         out_specs=row_spec, check_vma=False)
```

```python
import functools

import jax
import jax.numpy as jnp
from jax import lax
from jax.experimental import pallas as pl
from jax.experimental.pallas import tpu as pltpu
from jax.sharding import PartitionSpec as P

MESH = pl.DeviceIdType.MESH
F32 = jnp.float32
BF16 = jnp.bfloat16
LANES = 128
CHIPS = 4
AHEAD = 2
STAGES = 4
GROUP = 3
LAG = 3


def slot_bound(n_tok, n_top, n_dev, n_slot):
    base_load = (n_tok * n_top) // (n_dev * n_slot)
    return base_load + base_load // 2 + 1


def round_up(n, m):
    return -(-n // m) * m


def gelu(v):
    return v * (0.5 + 0.5 * jnp.tanh(v * (0.7978845608028654 + (0.7978845608028654 * 0.044715) * (v * v))))


def dot(a, b):
    return lax.dot_general(a, b, (((1,), (0,)), ((), ())), preferred_element_type=F32)


def moe_kernel(cfg, x_ref, idx_ref, gate_ref, tab_ref, wup_ref, wdn_ref, y_ref,
               xall, idx_all, gate_all, trk, g_buf, c_buf, xg, acc, h_buf, o_buf, wu, wd, sib_in, far_in, dir_in, mrg_in,
               meta_ss, meta_rs, near_ss, near_rs, rel_ss, rel_rs, sib_ss, sib_rs, wu_s, wd_s,
               ps_ss, ps_rs, pf_ss, pf_rs, pd_ss, pd_rs, pm_ss, pm_rs):
    bound, cap, kb_w, cb_w = (cfg[k] for k in ("bound", "cap", "kb_w", "cb_w"))
    n_tok, d_model = x_ref.shape
    n_top = idx_ref.shape[0]
    n_dev, n_slot = tab_ref.shape
    d_ff = wup_ref.shape[-1]
    d_mid = n_dev * cap
    n_kb, n_cb = d_model // kb_w, d_model // cb_w
    half = n_tok // 2
    me = lax.axis_index("ep")
    chip, core = me // 2, me % 2

    def dev(d_chip, d_core=0):
        return {"ep": ((chip + d_chip) % CHIPS) * 2 + (core + d_core) % 2}

    right, left, sib = dev(1), dev(CHIPS - 1), dev(0, 1)

    def rcopy(src, dst, ss, rs, to):
        return pltpu.make_async_remote_copy(src_ref=src, dst_ref=dst, send_sem=ss, recv_sem=rs, device_id=to, device_id_type=MESH)

    def up_load(kb, s):
        return pltpu.make_async_copy(wup_ref.at[0, s, pl.ds(pl.multiple_of(kb * kb_w, kb_w), kb_w), :], wu.at[s], wu_s.at[s])

    def down_load(cb, s):
        return pltpu.make_async_copy(wdn_ref.at[0, s, :, pl.ds(cb * cb_w, cb_w)], wd.at[s], wd_s.at[s])

    barrier = pltpu.get_barrier_semaphore()
    peers = [(dx, dc) for dx in range(CHIPS) for dc in range(2) if dx or dc]
    for dx, dc in peers:
        pl.semaphore_signal(barrier, inc=1, device_id=dev(dx, dc), device_id_type=MESH)
    for s in range(n_slot):
        up_load(0, s).start()
    pl.semaphore_wait(barrier, len(peers))

    lo, hi = pl.ds(0, half), pl.ds(half, n_tok - half)
    prev = CHIPS - 1

    def own(kb):
        return x_ref.at[:, pl.ds(pl.multiple_of(kb * kb_w, kb_w), kb_w)]

    def near(kb):
        return (rcopy(own(kb), xall.at[2 * prev, kb], near_ss.at[kb, 0], near_rs.at[kb, 0], right),
                rcopy(own(kb), xall.at[2, kb], near_ss.at[kb, 1], near_rs.at[kb, 1], left))

    def relay(kb):
        return (rcopy(xall.at[2 * prev, kb, lo], xall.at[4, kb, lo], rel_ss.at[kb, 0], rel_rs.at[kb, 0], right),
                rcopy(xall.at[2, kb, hi], xall.at[4, kb, hi], rel_ss.at[kb, 1], rel_rs.at[kb, 1], left))

    def across(kb, off):
        return rcopy(xall.at[2 * off, kb] if off else own(kb), xall.at[2 * off + 1, kb], sib_ss.at[kb, off], sib_rs.at[kb, off], sib)

    def start_near(kb):
        for c in near(kb):
            c.start()

    def stage_near(kb):
        for c, r, off in zip(near(kb), relay(kb), (prev, 1)):
            c.wait_recv()
            r.start()
            across(kb, off).start()

    def stage_far(kb):
        for r in relay(kb):
            r.wait_recv()
        across(kb, 2).start()

    metas = []
    for n, (dx, dc) in enumerate(peers):
        place = 2 * ((CHIPS - dx) % CHIPS) + dc
        metas.append(rcopy(idx_ref, idx_all.at[place], meta_ss.at[n, 0], meta_rs.at[n, 0], dev(dx, dc)))
        metas.append(rcopy(gate_ref, gate_all.at[place], meta_ss.at[n, 1], meta_rs.at[n, 1], dev(dx, dc)))
    start_near(0)
    for m in metas:
        m.start()
    for kb in range(1, AHEAD):
        start_near(kb)
    for kb in range(n_kb):
        across(kb, 0).start()
    for s in range(n_slot):
        down_load(0, s).start()

    idx_all[0] = idx_ref[...]
    gate_all[0] = gate_ref[...]
    for kb in range(n_kb):
        xall[0, kb] = x_ref[:, kb * kb_w:(kb + 1) * kb_w]

    rows_s = round_up(n_slot, 8)
    sub = lax.broadcasted_iota(jnp.int32, (rows_s, n_slot), 0)
    lane = lax.broadcasted_iota(jnp.int32, (rows_s, n_slot), 1)
    my_row = tab_ref[pl.ds(me, 1), :].astype(F32)
    e_col = jnp.sum(jnp.where(sub == lane, my_row, 0.0), axis=1, keepdims=True)
    e_col = jnp.where(sub[:, 0:1] < n_slot, e_col, -2.0)
    total = jnp.zeros((rows_s, n_slot), F32)
    before = jnp.zeros((rows_s, n_slot), F32)
    for d in range(n_dev):
        same = jnp.where(tab_ref[d:d + 1, :].astype(F32) == e_col, 1.0, 0.0)
        total = total + same
        before = before + same * jnp.where(d < me, 1.0, 0.0)
    copies = jnp.sum(total, axis=1, keepdims=True)
    my_rank = jnp.sum(before, axis=1, keepdims=True)
    r = lax.broadcasted_iota(jnp.int32, (cap, LANES), 0)
    for s in range(n_slot):
        want = r.astype(F32) * copies[s:s + 1, :] + my_rank[s:s + 1, :]
        trk[s * cap:(s + 1) * cap, :] = jnp.where(r < bound, want, -2.0)

    def clear(q, carry):
        acc[q] = jnp.zeros(acc.shape[1:], F32)
        return carry

    lax.fori_loop(0, acc.shape[0], clear, 0)
    stage_near(0)
    start_near(AHEAD)

    for m in metas:
        m.wait_recv()
    lane_tok = n_tok
    earlier = (lax.broadcasted_iota(jnp.int32, (lane_tok, lane_tok), 0)
               < lax.broadcasted_iota(jnp.int32, (lane_tok, lane_tok), 1)).astype(F32).astype(BF16)
    rows_src = n_slot * cap
    rows_pad = round_up(rows_src, LANES)

    def route(j, carry):
        idx = idx_all[j].astype(F32)
        gates = gate_all[j]
        has = jnp.zeros((rows_s, lane_tok), F32)
        gate = jnp.zeros((rows_s, lane_tok), F32)
        for q in range(n_top):
            hit = idx[q:q + 1, :] == e_col
            has = jnp.where(hit, 1.0, has)
            gate = jnp.where(hit, gates[q:q + 1, :], gate)
        rank = jnp.where(has > 0.0, dot(has.astype(BF16), earlier), -1.0)
        parts = []
        for s in range(n_slot):
            hit = rank[s:s + 1, :] == trk[s * cap:(s + 1) * cap, 0:1]
            g_buf[j, s * cap:(s + 1) * cap, :] = jnp.where(hit, 1.0, 0.0).astype(BF16)
            parts.append(jnp.where(hit, gate[s:s + 1, :], 0.0))
        if rows_pad > rows_src:
            parts.append(jnp.zeros((rows_pad - rows_src, lane_tok), F32))
        left_over = jnp.transpose(jnp.concatenate(parts, axis=0))[:, :rows_src]
        for n in range(3):
            term = left_over.astype(BF16)
            c_buf[j, n * n_tok:(n + 1) * n_tok, :] = term
            left_over = left_over - term.astype(F32)
        return carry

    lax.fori_loop(0, n_dev, route, 0)
    stage_near(1)
    start_near(AHEAD + 1)
    stage_far(0)

    chunks = [(n, min(2 * LANES, d_ff - n)) for n in range(0, d_ff, 2 * LANES)]
    n_mid = d_ff // LANES
    groups = [range(s, min(s + GROUP, n_slot)) for s in range(0, n_slot, GROUP)]

    def up_block(kb, last, after):
        for off in range(CHIPS):
            across(kb, off).wait_recv()

        def gather(j, carry):
            rows = dot(g_buf[j], xall[j, kb]).astype(BF16)
            for s in range(n_slot):
                xg[s, pl.ds(pl.multiple_of(j * cap, cap), cap), :] = rows[s * cap:(s + 1) * cap]
            return carry

        lax.fori_loop(0, n_dev, gather, 0)
        for g, group in enumerate(groups):
            for s in group:
                up_load(kb, s).wait()
            for s in group:
                for n0, nw in chunks:
                    v = dot(xg[s], wu[s, :, n0:n0 + nw])
                    for n in range(0, nw, LANES):
                        q = s * n_mid + (n0 + n) // LANES
                        part = acc[q, :d_mid, :] + v[:, n:n + LANES]
                        if last:
                            h_buf[s, :, n0 + n:n0 + n + LANES] = gelu(part).astype(BF16)
                        else:
                            acc[q, :d_mid, :] = part
            if not last:
                for s in group:
                    up_load(kb + 1, s).start()
            if g in after:
                after[g]()

    def up_step(kb, carry):
        def near_2():
            @pl.when(kb + 2 < n_kb)
            def _():
                stage_near(kb + 2)

            @pl.when(kb + 2 + AHEAD < n_kb)
            def _():
                start_near(kb + 2 + AHEAD)

        up_block(kb, False, {0: near_2, 1: lambda: stage_far(kb + 1)})
        return carry

    lax.fori_loop(0, n_kb - 1, up_step, 0)
    up_block(n_kb - 1, True, {})

    def mine(cb, off, h):
        return (cb * CHIPS + off) * 2 + h

    def staged(cb, off, h):
        return n_cb * CHIPS * 2 + ((cb % STAGES) * CHIPS + off) * 2 + h

    tok = pl.ds(0, n_tok)
    to_sib = [[rcopy(acc.at[pl.ds(staged(cb, off, 0), 2), tok], sib_in.at[cb, off], ps_ss.at[cb, off], ps_rs.at[cb, off], sib)
               for off in range(CHIPS)] for cb in range(n_cb)]
    to_far = [(rcopy(acc.at[mine(cb, 2, 0), tok], far_in.at[cb, 0], pf_ss.at[cb, 0], pf_rs.at[cb, 0], right),
               rcopy(acc.at[mine(cb, 2, 1), tok], far_in.at[cb, 1], pf_ss.at[cb, 1], pf_rs.at[cb, 1], left)) for cb in range(n_cb)]
    to_dir = [(rcopy(acc.at[mine(cb, 1, 1), tok], dir_in.at[cb, 0], pd_ss.at[cb, 0], pd_rs.at[cb, 0], right),
               rcopy(acc.at[mine(cb, 3, 0), tok], dir_in.at[cb, 1], pd_ss.at[cb, 1], pd_rs.at[cb, 1], left)) for cb in range(n_cb)]
    to_mrg = [(rcopy(far_in.at[cb, 0], mrg_in.at[cb, 0], pm_ss.at[cb, 0], pm_rs.at[cb, 0], right),
               rcopy(far_in.at[cb, 1], mrg_in.at[cb, 1], pm_ss.at[cb, 1], pm_rs.at[cb, 1], left)) for cb in range(n_cb)]

    def merge(cb):
        to_far[cb][0].wait_recv()
        far_in[cb, 0] = far_in[cb, 0] + acc[mine(cb, 1, 0), :n_tok, :]
        to_mrg[cb][0].start()
        to_far[cb][1].wait_recv()
        far_in[cb, 1] = far_in[cb, 1] + acc[mine(cb, 3, 1), :n_tok, :]
        to_mrg[cb][1].start()

    def finish(cb):
        for h in range(2):
            to_mrg[cb][h].wait_recv()
            to_dir[cb][1 - h].wait_recv()
            out = acc[mine(cb, 0, h), :n_tok, :] + mrg_in[cb, h] + dir_in[cb, 1 - h]
            y_ref[:, cb * cb_w + h * LANES:cb * cb_w + (h + 1) * LANES] = out.astype(BF16)

    for cb in range(n_cb):
        def down(s, carry, cb=cb):
            down_load(cb, s).wait()
            out = dot(h_buf[s], wd[s]).astype(BF16)
            for j in range(n_dev):
                o_buf[j, pl.ds(pl.multiple_of(s * cap, cap), cap), :] = out[j * cap:(j + 1) * cap]
            if cb + 1 < n_cb:
                down_load(cb + 1, s).start()
            return carry

        lax.fori_loop(0, n_slot, down, 0)
        if cb >= STAGES:
            for off in range(CHIPS):
                to_sib[cb - STAGES][off].wait_send()

        def combine(off, carry, dc, first):
            v = dot(c_buf[2 * off + dc], o_buf[2 * off + dc])
            v = (v[2 * n_tok:] + v[n_tok:2 * n_tok]) + v[:n_tok]
            acc[first + 2 * off, :n_tok, :] = v[:, :LANES]
            acc[first + 2 * off + 1, :n_tok, :] = v[:, LANES:]
            return carry

        lax.fori_loop(0, CHIPS, functools.partial(combine, dc=1, first=staged(cb, 0, 0)), 0)
        for off in (2, 1, 3, 0):
            to_sib[cb][off].start()
        lax.fori_loop(0, CHIPS, functools.partial(combine, dc=0, first=mine(cb, 0, 0)), 0)
        if cb >= LAG:
            finish(cb - LAG)
        for off in (2, 1, 3, 0):
            to_sib[cb][off].wait_recv()
            for h in range(2):
                q = mine(cb, off, h)
                acc[q, :n_tok, :] = acc[q, :n_tok, :] + sib_in[cb, off, h]
            if off == 2:
                to_far[cb][0].start()
                to_far[cb][1].start()
            elif off:
                to_dir[cb][0 if off == 1 else 1].start()
        if cb >= 1:
            merge(cb - 1)
    merge(n_cb - 1)
    for cb in range(max(0, n_cb - LAG), n_cb):
        finish(cb)

    for m in metas:
        m.wait_send()

    def drain(kb, carry):
        for c in near(kb) + relay(kb) + tuple(across(kb, off) for off in range(CHIPS)):
            c.wait_send()
        return carry

    lax.fori_loop(0, n_kb, drain, 0)
    for cb in range(n_cb):
        for c in to_far[cb] + to_dir[cb] + to_mrg[cb]:
            c.wait_send()
        if cb + STAGES >= n_cb:
            for c in to_sib[cb]:
                c.wait_send()


def solution(mesh):
    assert mesh.shape["ep"] == 2 * CHIPS

    def group_layer(tokens, topk_idx, topk_w, w_up, w_down, slot_expert):
        n_tok, d_model = tokens.shape
        n_top = topk_idx.shape[1]
        n_dev, n_slot = slot_expert.shape
        d_ff = w_up.shape[-1]
        bound = slot_bound(n_tok, n_top, n_dev, n_slot)
        cap = round_up(bound, 16)
        kb_w, cb_w = 2 * LANES, 2 * LANES
        n_kb, n_cb = d_model // kb_w, d_model // cb_w
        d_mid = n_dev * cap
        rows_src = n_slot * cap
        n_acc = max(n_slot * (d_ff // LANES), (n_cb + STAGES) * CHIPS * 2)
        cfg = dict(bound=bound, cap=cap, kb_w=kb_w, cb_w=cb_w)
        dma = pltpu.SemaphoreType.DMA
        vmem = pl.BlockSpec(memory_space=pltpu.VMEM)
        hbm = pl.BlockSpec(memory_space=pl.ANY)
        return pl.pallas_call(
            functools.partial(moe_kernel, cfg),
            out_shape=jax.ShapeDtypeStruct((n_tok, d_model), BF16),
            in_specs=[vmem, vmem, vmem, vmem, hbm, hbm],
            out_specs=vmem,
            scratch_shapes=[
                pltpu.VMEM((n_dev, n_kb, n_tok, kb_w), BF16),
                pltpu.VMEM((n_dev, n_top, n_tok), jnp.int32),
                pltpu.VMEM((n_dev, n_top, n_tok), F32),
                pltpu.VMEM((rows_src, LANES), F32),
                pltpu.VMEM((n_dev, rows_src, n_tok), BF16),
                pltpu.VMEM((n_dev, 3 * n_tok, rows_src), BF16),
                pltpu.VMEM((n_slot, d_mid, kb_w), BF16),
                pltpu.VMEM((n_acc, max(d_mid, n_tok), LANES), F32),
                pltpu.VMEM((n_slot, d_mid, d_ff), BF16),
                pltpu.VMEM((n_dev, rows_src, cb_w), BF16),
                pltpu.VMEM((n_slot, kb_w, d_ff), BF16),
                pltpu.VMEM((n_slot, d_ff, cb_w), BF16),
                pltpu.VMEM((n_cb, CHIPS, 2, n_tok, LANES), F32),
                pltpu.VMEM((n_cb, 2, n_tok, LANES), F32),
                pltpu.VMEM((n_cb, 2, n_tok, LANES), F32),
                pltpu.VMEM((n_cb, 2, n_tok, LANES), F32),
                dma((n_dev - 1, 2)), dma((n_dev - 1, 2)),
                dma((n_kb, 2)), dma((n_kb, 2)), dma((n_kb, 2)), dma((n_kb, 2)),
                dma((n_kb, CHIPS)), dma((n_kb, CHIPS)),
                dma((n_slot,)), dma((n_slot,)),
                dma((n_cb, CHIPS)), dma((n_cb, CHIPS)),
                dma((n_cb, 2)), dma((n_cb, 2)), dma((n_cb, 2)), dma((n_cb, 2)), dma((n_cb, 2)), dma((n_cb, 2)),
            ],
            compiler_params=pltpu.CompilerParams(collective_id=0, has_side_effects=True, vmem_limit_bytes=67_000_000),
        )(tokens, topk_idx.T, topk_w.T, slot_expert, w_up, w_down)

    row_spec = P(('dp', 'ep'), None)
    weight_spec = P('ep', None, None, None)
    return jax.shard_map(group_layer, mesh=mesh, in_specs=(row_spec, row_spec, row_spec, weight_spec, weight_spec, P(None, None)),
                         out_specs=row_spec, check_vma=False)
```

```python
import functools

import jax
import jax.numpy as jnp
from jax import lax
from jax.experimental import pallas as pl
from jax.experimental.pallas import tpu as pltpu
from jax.sharding import PartitionSpec as P

MESH = pl.DeviceIdType.MESH
F32 = jnp.float32
BF16 = jnp.bfloat16
LANES = 128
CHIPS = 4
AHEAD = 2
STAGES = 4
GROUP = 3
LAG = 3


def slot_bound(n_tok, n_top, n_dev, n_slot):
    base_load = (n_tok * n_top) // (n_dev * n_slot)
    return base_load + base_load // 2 + 1


def round_up(n, m):
    return -(-n // m) * m


def gelu(v):
    return v * (0.5 + 0.5 * jnp.tanh(v * (0.7978845608028654 + (0.7978845608028654 * 0.044715) * (v * v))))


def dot(a, b):
    return lax.dot_general(a, b, (((1,), (0,)), ((), ())), preferred_element_type=F32)


def moe_kernel(cfg, x_ref, idx_ref, gate_ref, tab_ref, wup_ref, wdn_ref, y_ref,
               xall, idx_all, gate_all, trk, g_buf, c_buf, xg, acc, h_buf, o_buf, wu, wd, sib_in, far_in, dir_in, mrg_in,
               meta_ss, meta_rs, near_ss, near_rs, rel_ss, rel_rs, sib_ss, sib_rs, wu_s, wd_s,
               ps_ss, ps_rs, pf_ss, pf_rs, pd_ss, pd_rs, pm_ss, pm_rs):
    bound, cap, kb_w, cb_w = (cfg[k] for k in ("bound", "cap", "kb_w", "cb_w"))
    n_tok, d_model = x_ref.shape
    n_top = idx_ref.shape[0]
    n_dev, n_slot = tab_ref.shape
    d_ff = wup_ref.shape[-1]
    d_mid = n_dev * cap
    n_kb, n_cb = d_model // kb_w, d_model // cb_w
    half = n_tok // 2
    me = lax.axis_index("ep")
    chip, core = me // 2, me % 2

    def dev(d_chip, d_core=0):
        return {"ep": ((chip + d_chip) % CHIPS) * 2 + (core + d_core) % 2}

    right, left, sib = dev(1), dev(CHIPS - 1), dev(0, 1)

    def rcopy(src, dst, ss, rs, to):
        return pltpu.make_async_remote_copy(src_ref=src, dst_ref=dst, send_sem=ss, recv_sem=rs, device_id=to, device_id_type=MESH)

    def up_load(kb, s):
        return pltpu.make_async_copy(wup_ref.at[0, s, pl.ds(pl.multiple_of(kb * kb_w, kb_w), kb_w), :], wu.at[s], wu_s.at[s])

    def down_load(cb, s):
        return pltpu.make_async_copy(wdn_ref.at[0, s, :, pl.ds(pl.multiple_of(cb * cb_w, cb_w), cb_w)], wd.at[s], wd_s.at[s])

    barrier = pltpu.get_barrier_semaphore()
    peers = [(dx, dc) for dx in range(CHIPS) for dc in range(2) if dx or dc]
    for dx, dc in peers:
        pl.semaphore_signal(barrier, inc=1, device_id=dev(dx, dc), device_id_type=MESH)
    for s in range(n_slot):
        up_load(0, s).start()
    pl.semaphore_wait(barrier, len(peers))

    lo, hi = pl.ds(0, half), pl.ds(half, n_tok - half)
    prev = CHIPS - 1

    def own(kb):
        return x_ref.at[:, pl.ds(pl.multiple_of(kb * kb_w, kb_w), kb_w)]

    def near(kb):
        return (rcopy(own(kb), xall.at[2 * prev, kb], near_ss.at[kb, 0], near_rs.at[kb, 0], right),
                rcopy(own(kb), xall.at[2, kb], near_ss.at[kb, 1], near_rs.at[kb, 1], left))

    def relay(kb):
        return (rcopy(xall.at[2 * prev, kb, lo], xall.at[4, kb, lo], rel_ss.at[kb, 0], rel_rs.at[kb, 0], right),
                rcopy(xall.at[2, kb, hi], xall.at[4, kb, hi], rel_ss.at[kb, 1], rel_rs.at[kb, 1], left))

    def across(kb, off):
        return rcopy(xall.at[2 * off, kb] if off else own(kb), xall.at[2 * off + 1, kb], sib_ss.at[kb, off], sib_rs.at[kb, off], sib)

    def start_near(kb):
        for c in near(kb):
            c.start()

    def stage_near(kb):
        for c, r, off in zip(near(kb), relay(kb), (prev, 1)):
            c.wait_recv()
            r.start()
            across(kb, off).start()

    def stage_far(kb):
        for r in relay(kb):
            r.wait_recv()
        across(kb, 2).start()

    metas = []
    for n, (dx, dc) in enumerate(peers):
        place = 2 * ((CHIPS - dx) % CHIPS) + dc
        metas.append(rcopy(idx_ref, idx_all.at[place], meta_ss.at[n, 0], meta_rs.at[n, 0], dev(dx, dc)))
        metas.append(rcopy(gate_ref, gate_all.at[place], meta_ss.at[n, 1], meta_rs.at[n, 1], dev(dx, dc)))
    start_near(0)
    for m in metas:
        m.start()
    for kb in range(1, AHEAD):
        start_near(kb)
    for kb in range(n_kb):
        across(kb, 0).start()
    for s in range(n_slot):
        down_load(0, s).start()

    idx_all[0] = idx_ref[...]
    gate_all[0] = gate_ref[...]
    for kb in range(n_kb):
        xall[0, kb] = x_ref[:, kb * kb_w:(kb + 1) * kb_w]

    rows_s = round_up(n_slot, 8)
    sub = lax.broadcasted_iota(jnp.int32, (rows_s, n_slot), 0)
    lane = lax.broadcasted_iota(jnp.int32, (rows_s, n_slot), 1)
    my_row = tab_ref[pl.ds(me, 1), :].astype(F32)
    e_col = jnp.sum(jnp.where(sub == lane, my_row, 0.0), axis=1, keepdims=True)
    e_col = jnp.where(sub[:, 0:1] < n_slot, e_col, -2.0)
    total = jnp.zeros((rows_s, n_slot), F32)
    before = jnp.zeros((rows_s, n_slot), F32)
    for d in range(n_dev):
        same = jnp.where(tab_ref[d:d + 1, :].astype(F32) == e_col, 1.0, 0.0)
        total = total + same
        before = before + same * jnp.where(d < me, 1.0, 0.0)
    copies = jnp.sum(total, axis=1, keepdims=True)
    my_rank = jnp.sum(before, axis=1, keepdims=True)
    r = lax.broadcasted_iota(jnp.int32, (cap, LANES), 0)
    for s in range(n_slot):
        want = r.astype(F32) * copies[s:s + 1, :] + my_rank[s:s + 1, :]
        trk[s * cap:(s + 1) * cap, :] = jnp.where(r < bound, want, -2.0)

    def clear(q, carry):
        acc[q] = jnp.zeros(acc.shape[1:], F32)
        return carry

    lax.fori_loop(0, acc.shape[0], clear, 0)
    stage_near(0)
    start_near(AHEAD)

    for m in metas:
        m.wait_recv()
    lane_tok = n_tok
    earlier = (lax.broadcasted_iota(jnp.int32, (lane_tok, lane_tok), 0)
               < lax.broadcasted_iota(jnp.int32, (lane_tok, lane_tok), 1)).astype(F32).astype(BF16)
    rows_src = n_slot * cap
    rows_pad = round_up(rows_src, LANES)

    def route(j, carry):
        idx = idx_all[j].astype(F32)
        gates = gate_all[j]
        has = jnp.zeros((rows_s, lane_tok), F32)
        gate = jnp.zeros((rows_s, lane_tok), F32)
        for q in range(n_top):
            hit = idx[q:q + 1, :] == e_col
            has = jnp.where(hit, 1.0, has)
            gate = jnp.where(hit, gates[q:q + 1, :], gate)
        rank = jnp.where(has > 0.0, dot(has.astype(BF16), earlier), -1.0)
        parts = []
        for s in range(n_slot):
            hit = rank[s:s + 1, :] == trk[s * cap:(s + 1) * cap, 0:1]
            g_buf[j, s * cap:(s + 1) * cap, :] = jnp.where(hit, 1.0, 0.0).astype(BF16)
            parts.append(jnp.where(hit, gate[s:s + 1, :], 0.0))
        if rows_pad > rows_src:
            parts.append(jnp.zeros((rows_pad - rows_src, lane_tok), F32))
        left_over = jnp.transpose(jnp.concatenate(parts, axis=0))[:, :rows_src]
        for n in range(3):
            term = left_over.astype(BF16)
            c_buf[j, n * n_tok:(n + 1) * n_tok, :] = term
            left_over = left_over - term.astype(F32)
        return carry

    lax.fori_loop(0, n_dev, route, 0)
    stage_near(1)
    start_near(AHEAD + 1)
    stage_far(0)

    chunks = [(n, min(2 * LANES, d_ff - n)) for n in range(0, d_ff, 2 * LANES)]
    n_mid = d_ff // LANES
    groups = [range(s, min(s + GROUP, n_slot)) for s in range(0, n_slot, GROUP)]

    def up_block(kb, last, after):
        for off in range(CHIPS):
            across(kb, off).wait_recv()

        for j in range(n_dev):
            rows = dot(g_buf[j], xall[j, kb]).astype(BF16)
            for s in range(n_slot):
                xg[s, j * cap:(j + 1) * cap, :] = rows[s * cap:(s + 1) * cap]
        for g, group in enumerate(groups):
            for s in group:
                up_load(kb, s).wait()
            for s in group:
                for n0, nw in chunks:
                    v = dot(xg[s], wu[s, :, n0:n0 + nw])
                    for n in range(0, nw, LANES):
                        q = s * n_mid + (n0 + n) // LANES
                        part = acc[q, :d_mid, :] + v[:, n:n + LANES]
                        if last:
                            h_buf[s, :, n0 + n:n0 + n + LANES] = gelu(part).astype(BF16)
                        else:
                            acc[q, :d_mid, :] = part
            if not last:
                for s in group:
                    up_load(kb + 1, s).start()
            if g in after:
                after[g]()

    def up_step(kb, carry):
        def near_2():
            @pl.when(kb + 2 < n_kb)
            def _():
                stage_near(kb + 2)

            @pl.when(kb + 2 + AHEAD < n_kb)
            def _():
                start_near(kb + 2 + AHEAD)

        up_block(kb, False, {0: near_2, 1: lambda: stage_far(kb + 1)})
        return carry

    lax.fori_loop(0, n_kb - 1, up_step, 0)
    up_block(n_kb - 1, True, {})

    def mine(cb, off, h):
        return (cb * CHIPS + off) * 2 + h

    def staged(cb, off, h):
        return n_cb * CHIPS * 2 + ((cb % STAGES) * CHIPS + off) * 2 + h

    tok = pl.ds(0, n_tok)

    def to_sib(cb, off):
        return rcopy(acc.at[pl.ds(staged(cb, off, 0), 2), tok], sib_in.at[cb, off], ps_ss.at[cb, off], ps_rs.at[cb, off], sib)

    def to_far(cb):
        return (rcopy(acc.at[mine(cb, 2, 0), tok], far_in.at[cb, 0], pf_ss.at[cb, 0], pf_rs.at[cb, 0], right),
                rcopy(acc.at[mine(cb, 2, 1), tok], far_in.at[cb, 1], pf_ss.at[cb, 1], pf_rs.at[cb, 1], left))

    def to_dir(cb):
        return (rcopy(acc.at[mine(cb, 1, 1), tok], dir_in.at[cb, 0], pd_ss.at[cb, 0], pd_rs.at[cb, 0], right),
                rcopy(acc.at[mine(cb, 3, 0), tok], dir_in.at[cb, 1], pd_ss.at[cb, 1], pd_rs.at[cb, 1], left))

    def to_mrg(cb):
        return (rcopy(far_in.at[cb, 0], mrg_in.at[cb, 0], pm_ss.at[cb, 0], pm_rs.at[cb, 0], right),
                rcopy(far_in.at[cb, 1], mrg_in.at[cb, 1], pm_ss.at[cb, 1], pm_rs.at[cb, 1], left))

    def merge(cb):
        for h, off in ((0, 1), (1, prev)):
            to_far(cb)[h].wait_recv()
            far_in[cb, h] = far_in[cb, h] + acc[mine(cb, off, h), :n_tok, :]
            to_mrg(cb)[h].start()

    def finish(cb):
        for h in range(2):
            to_mrg(cb)[h].wait_recv()
            to_dir(cb)[1 - h].wait_recv()
            out = acc[mine(cb, 0, h), :n_tok, :] + mrg_in[cb, h] + dir_in[cb, 1 - h]
            y_ref[:, pl.ds(pl.multiple_of(cb * cb_w + h * LANES, LANES), LANES)] = out.astype(BF16)

    def combine(j, q):
        v = dot(c_buf[j], o_buf[j])
        v = (v[2 * n_tok:] + v[n_tok:2 * n_tok]) + v[:n_tok]
        for h in range(2):
            acc[q + h, :n_tok, :] = v[:, h * LANES:(h + 1) * LANES]

    def down_step(cb, carry):
        for group in groups:
            for s in group:
                down_load(cb, s).wait()
            for s in group:
                out = dot(h_buf[s], wd[s]).astype(BF16)
                for j in range(n_dev):
                    o_buf[j, s * cap:(s + 1) * cap, :] = out[j * cap:(j + 1) * cap]

            @pl.when(cb + 1 < n_cb)
            def _():
                for s in group:
                    down_load(cb + 1, s).start()

        @pl.when(cb >= STAGES)
        def _():
            for off in range(CHIPS):
                to_sib(cb - STAGES, off).wait_send()

        order = (2, 1, prev, 0)
        for off in order:
            combine(2 * off + 1, staged(cb, off, 0))
            to_sib(cb, off).start()
        for off in order:
            combine(2 * off, mine(cb, off, 0))

        @pl.when(cb >= LAG)
        def _():
            finish(cb - LAG)

        for off in order:
            to_sib(cb, off).wait_recv()
            for h in range(2):
                q = mine(cb, off, h)
                acc[q, :n_tok, :] = acc[q, :n_tok, :] + sib_in[cb, off, h]
            if off == 2:
                for c in to_far(cb):
                    c.start()
            elif off:
                to_dir(cb)[0 if off == 1 else 1].start()

        @pl.when(cb >= 1)
        def _():
            merge(cb - 1)
        return carry

    lax.fori_loop(0, n_cb, down_step, 0)
    merge(n_cb - 1)
    for cb in range(max(0, n_cb - LAG), n_cb):
        finish(cb)

    for m in metas:
        m.wait_send()

    def drain(kb, carry):
        for c in near(kb) + relay(kb) + tuple(across(kb, off) for off in range(CHIPS)):
            c.wait_send()
        return carry

    lax.fori_loop(0, n_kb, drain, 0)

    def drain_sums(cb, carry):
        for c in to_far(cb) + to_dir(cb) + to_mrg(cb):
            c.wait_send()
        return carry

    lax.fori_loop(0, n_cb, drain_sums, 0)
    for cb in range(max(0, n_cb - STAGES), n_cb):
        for off in range(CHIPS):
            to_sib(cb, off).wait_send()


def solution(mesh):
    assert mesh.shape["ep"] == 2 * CHIPS

    def group_layer(tokens, topk_idx, topk_w, w_up, w_down, slot_expert):
        n_tok, d_model = tokens.shape
        n_top = topk_idx.shape[1]
        n_dev, n_slot = slot_expert.shape
        d_ff = w_up.shape[-1]
        bound = slot_bound(n_tok, n_top, n_dev, n_slot)
        cap = round_up(bound, 16)
        kb_w, cb_w = 2 * LANES, 2 * LANES
        n_kb, n_cb = d_model // kb_w, d_model // cb_w
        d_mid = n_dev * cap
        rows_src = n_slot * cap
        n_acc = max(n_slot * (d_ff // LANES), (n_cb + STAGES) * CHIPS * 2)
        cfg = dict(bound=bound, cap=cap, kb_w=kb_w, cb_w=cb_w)
        dma = pltpu.SemaphoreType.DMA
        vmem = pl.BlockSpec(memory_space=pltpu.VMEM)
        hbm = pl.BlockSpec(memory_space=pl.ANY)
        return pl.pallas_call(
            functools.partial(moe_kernel, cfg),
            out_shape=jax.ShapeDtypeStruct((n_tok, d_model), BF16),
            in_specs=[vmem, vmem, vmem, vmem, hbm, hbm],
            out_specs=vmem,
            scratch_shapes=[
                pltpu.VMEM((n_dev, n_kb, n_tok, kb_w), BF16),
                pltpu.VMEM((n_dev, n_top, n_tok), jnp.int32),
                pltpu.VMEM((n_dev, n_top, n_tok), F32),
                pltpu.VMEM((rows_src, LANES), F32),
                pltpu.VMEM((n_dev, rows_src, n_tok), BF16),
                pltpu.VMEM((n_dev, 3 * n_tok, rows_src), BF16),
                pltpu.VMEM((n_slot, d_mid, kb_w), BF16),
                pltpu.VMEM((n_acc, max(d_mid, n_tok), LANES), F32),
                pltpu.VMEM((n_slot, d_mid, d_ff), BF16),
                pltpu.VMEM((n_dev, rows_src, cb_w), BF16),
                pltpu.VMEM((n_slot, kb_w, d_ff), BF16),
                pltpu.VMEM((n_slot, d_ff, cb_w), BF16),
                pltpu.VMEM((n_cb, CHIPS, 2, n_tok, LANES), F32),
                pltpu.VMEM((n_cb, 2, n_tok, LANES), F32),
                pltpu.VMEM((n_cb, 2, n_tok, LANES), F32),
                pltpu.VMEM((n_cb, 2, n_tok, LANES), F32),
                dma((n_dev - 1, 2)), dma((n_dev - 1, 2)),
                dma((n_kb, 2)), dma((n_kb, 2)), dma((n_kb, 2)), dma((n_kb, 2)),
                dma((n_kb, CHIPS)), dma((n_kb, CHIPS)),
                dma((n_slot,)), dma((n_slot,)),
                dma((n_cb, CHIPS)), dma((n_cb, CHIPS)),
                dma((n_cb, 2)), dma((n_cb, 2)), dma((n_cb, 2)), dma((n_cb, 2)), dma((n_cb, 2)), dma((n_cb, 2)),
            ],
            compiler_params=pltpu.CompilerParams(collective_id=0, has_side_effects=True, vmem_limit_bytes=67_000_000),
        )(tokens, topk_idx.T, topk_w.T, slot_expert, w_up, w_down)

    row_spec = P(('dp', 'ep'), None)
    weight_spec = P('ep', None, None, None)
    return jax.shard_map(group_layer, mesh=mesh, in_specs=(row_spec, row_spec, row_spec, weight_spec, weight_spec, P(None, None)),
                         out_specs=row_spec, check_vma=False)
```

```python
import functools

import jax
import jax.numpy as jnp
from jax import lax
from jax.experimental import pallas as pl
from jax.experimental.pallas import tpu as pltpu
from jax.sharding import PartitionSpec as P

MESH = pl.DeviceIdType.MESH
F32 = jnp.float32
BF16 = jnp.bfloat16
LANES = 128
CHIPS = 4
AHEAD = 2
STAGES = 4
GROUP = 3
LAG = 3


def slot_bound(n_tok, n_top, n_dev, n_slot):
    base_load = (n_tok * n_top) // (n_dev * n_slot)
    return base_load + base_load // 2 + 1


def round_up(n, m):
    return -(-n // m) * m


def gelu(v):
    return v * (0.5 + 0.5 * jnp.tanh(v * (0.7978845608028654 + (0.7978845608028654 * 0.044715) * (v * v))))


def dot(a, b):
    return lax.dot_general(a, b, (((1,), (0,)), ((), ())), preferred_element_type=F32)


def moe_kernel(cfg, x_ref, idx_ref, gate_ref, tab_ref, wup_ref, wdn_ref, y_ref,
               xall, idx_all, gate_all, trk, g_buf, c_buf, xg, xg_odd, acc, h_buf, o_buf, o_odd, wu, wd, sib_in, far_in, dir_in, mrg_in,
               meta_ss, meta_rs, near_ss, near_rs, rel_ss, rel_rs, sib_ss, sib_rs, wu_s, wd_s,
               ps_ss, ps_rs, pf_ss, pf_rs, pd_ss, pd_rs, pm_ss, pm_rs):
    bound, cap, kb_w, cb_w = (cfg[k] for k in ("bound", "cap", "kb_w", "cb_w"))
    odd = bound - cap
    n_tok, d_model = x_ref.shape
    n_top = idx_ref.shape[0]
    n_dev, n_slot = tab_ref.shape
    d_ff = wup_ref.shape[-1]
    d_main, d_mid = n_dev * cap, n_dev * bound
    rows_s = round_up(n_slot, 16)
    rows_main, rows_src = n_slot * cap, n_slot * cap + odd * rows_s
    n_kb, n_cb = d_model // kb_w, d_model // cb_w
    half = n_tok // 2
    me = lax.axis_index("ep")
    chip, core = me // 2, me % 2

    def dev(d_chip, d_core=0):
        return {"ep": ((chip + d_chip) % CHIPS) * 2 + (core + d_core) % 2}

    right, left, sib = dev(1), dev(CHIPS - 1), dev(0, 1)

    def rcopy(src, dst, ss, rs, to):
        return pltpu.make_async_remote_copy(src_ref=src, dst_ref=dst, send_sem=ss, recv_sem=rs, device_id=to, device_id_type=MESH)

    def up_load(kb, s):
        return pltpu.make_async_copy(wup_ref.at[0, s, pl.ds(pl.multiple_of(kb * kb_w, kb_w), kb_w), :], wu.at[s], wu_s.at[s])

    def down_load(cb, s):
        return pltpu.make_async_copy(wdn_ref.at[0, s, :, pl.ds(pl.multiple_of(cb * cb_w, cb_w), cb_w)], wd.at[s], wd_s.at[s])

    barrier = pltpu.get_barrier_semaphore()
    peers = [(dx, dc) for dx in range(CHIPS) for dc in range(2) if dx or dc]
    for dx, dc in peers:
        pl.semaphore_signal(barrier, inc=1, device_id=dev(dx, dc), device_id_type=MESH)
    for s in range(n_slot):
        up_load(0, s).start()
    pl.semaphore_wait(barrier, len(peers))

    lo, hi = pl.ds(0, half), pl.ds(half, n_tok - half)
    prev = CHIPS - 1

    def own(kb):
        return x_ref.at[:, pl.ds(pl.multiple_of(kb * kb_w, kb_w), kb_w)]

    def near(kb):
        return (rcopy(own(kb), xall.at[2 * prev, kb], near_ss.at[kb, 0], near_rs.at[kb, 0], right),
                rcopy(own(kb), xall.at[2, kb], near_ss.at[kb, 1], near_rs.at[kb, 1], left))

    def relay(kb):
        return (rcopy(xall.at[2 * prev, kb, lo], xall.at[4, kb, lo], rel_ss.at[kb, 0], rel_rs.at[kb, 0], right),
                rcopy(xall.at[2, kb, hi], xall.at[4, kb, hi], rel_ss.at[kb, 1], rel_rs.at[kb, 1], left))

    def across(kb, off):
        return rcopy(xall.at[2 * off, kb] if off else own(kb), xall.at[2 * off + 1, kb], sib_ss.at[kb, off], sib_rs.at[kb, off], sib)

    def start_near(kb):
        for c in near(kb):
            c.start()

    def stage_near(kb):
        for c, r, off in zip(near(kb), relay(kb), (prev, 1)):
            c.wait_recv()
            r.start()
            across(kb, off).start()

    def stage_far(kb):
        for r in relay(kb):
            r.wait_recv()
        across(kb, 2).start()

    metas = []
    for n, (dx, dc) in enumerate(peers):
        place = 2 * ((CHIPS - dx) % CHIPS) + dc
        metas.append(rcopy(idx_ref, idx_all.at[place], meta_ss.at[n, 0], meta_rs.at[n, 0], dev(dx, dc)))
        metas.append(rcopy(gate_ref, gate_all.at[place], meta_ss.at[n, 1], meta_rs.at[n, 1], dev(dx, dc)))
    start_near(0)
    for m in metas:
        m.start()
    for kb in range(1, AHEAD):
        start_near(kb)
    for kb in range(n_kb):
        across(kb, 0).start()
    for s in range(n_slot):
        down_load(0, s).start()

    idx_all[0] = idx_ref[...]
    gate_all[0] = gate_ref[...]
    for kb in range(n_kb):
        xall[0, kb] = x_ref[:, kb * kb_w:(kb + 1) * kb_w]

    sub = lax.broadcasted_iota(jnp.int32, (rows_s, n_slot), 0)
    lane = lax.broadcasted_iota(jnp.int32, (rows_s, n_slot), 1)
    my_row = tab_ref[pl.ds(me, 1), :].astype(F32)
    e_col = jnp.sum(jnp.where(sub == lane, my_row, 0.0), axis=1, keepdims=True)
    e_col = jnp.where(sub[:, 0:1] < n_slot, e_col, -2.0)
    total = jnp.zeros((rows_s, n_slot), F32)
    before = jnp.zeros((rows_s, n_slot), F32)
    for d in range(n_dev):
        same = jnp.where(tab_ref[d:d + 1, :].astype(F32) == e_col, 1.0, 0.0)
        total = total + same
        before = before + same * jnp.where(d < me, 1.0, 0.0)
    copies = jnp.sum(total, axis=1, keepdims=True)
    my_rank = jnp.sum(before, axis=1, keepdims=True)
    r = lax.broadcasted_iota(jnp.int32, (cap, LANES), 0)
    for s in range(n_slot):
        want = r.astype(F32) * copies[s:s + 1, :] + my_rank[s:s + 1, :]
        trk[s * cap:(s + 1) * cap, :] = want
    o_odd[...] = jnp.zeros_like(o_odd)

    def clear(q, carry):
        acc[q] = jnp.zeros(acc.shape[1:], F32)
        return carry

    lax.fori_loop(0, acc.shape[0], clear, 0)
    stage_near(0)
    start_near(AHEAD)

    for m in metas:
        m.wait_recv()
    lane_tok = n_tok
    earlier = (lax.broadcasted_iota(jnp.int32, (lane_tok, lane_tok), 0)
               < lax.broadcasted_iota(jnp.int32, (lane_tok, lane_tok), 1)).astype(F32).astype(BF16)
    rows_pad = round_up(rows_src, LANES)

    def route(j, carry):
        idx = idx_all[j].astype(F32)
        gates = gate_all[j]
        has = jnp.zeros((rows_s, lane_tok), F32)
        gate = jnp.zeros((rows_s, lane_tok), F32)
        for q in range(n_top):
            hit = idx[q:q + 1, :] == e_col
            has = jnp.where(hit, 1.0, has)
            gate = jnp.where(hit, gates[q:q + 1, :], gate)
        rank = jnp.where(has > 0.0, dot(has.astype(BF16), earlier), -1.0)
        parts = []
        for s in range(n_slot):
            hit = rank[s:s + 1, :] == trk[s * cap:(s + 1) * cap, 0:1]
            g_buf[j, s * cap:(s + 1) * cap, :] = jnp.where(hit, 1.0, 0.0).astype(BF16)
            parts.append(jnp.where(hit, gate[s:s + 1, :], 0.0))
        for n in range(odd):
            hit = rank == float(cap + n) * copies + my_rank
            first = rows_main + n * rows_s
            g_buf[j, first:first + rows_s, :] = jnp.where(hit, 1.0, 0.0).astype(BF16)
            parts.append(jnp.where(hit, gate, 0.0))
        if rows_pad > rows_src:
            parts.append(jnp.zeros((rows_pad - rows_src, lane_tok), F32))
        left_over = jnp.transpose(jnp.concatenate(parts, axis=0))[:, :rows_src]
        for n in range(3):
            term = left_over.astype(BF16)
            c_buf[j, n * n_tok:(n + 1) * n_tok, :] = term
            left_over = left_over - term.astype(F32)
        return carry

    lax.fori_loop(0, n_dev, route, 0)
    stage_near(1)
    start_near(AHEAD + 1)
    stage_far(0)

    chunks = [(n, min(2 * LANES, d_ff - n)) for n in range(0, d_ff, 2 * LANES)]
    n_mid = d_ff // LANES
    groups = [range(s, min(s + GROUP, n_slot)) for s in range(0, n_slot, GROUP)]

    def up_block(kb, last, after):
        for off in range(CHIPS):
            across(kb, off).wait_recv()

        for j in range(n_dev):
            rows = dot(g_buf[j], xall[j, kb])
            main = rows[:rows_main].astype(BF16)
            for s in range(n_slot):
                xg[s, j * cap:(j + 1) * cap, :] = main[s * cap:(s + 1) * cap]
            for n in range(odd):
                first = rows_main + n * rows_s
                for h in range(kb_w // LANES):
                    xg_odd[n, h, pl.ds(j, rows_s, stride=n_dev), :] = rows[first:first + rows_s, h * LANES:(h + 1) * LANES]
        for n in range(odd):
            for h in range(kb_w // LANES):
                for s in range(n_slot):
                    xg[s, d_main + n * n_dev:d_main + (n + 1) * n_dev, h * LANES:(h + 1) * LANES] = (
                        xg_odd[n, h, s * n_dev:(s + 1) * n_dev, :].astype(BF16))
        for g, group in enumerate(groups):
            for s in group:
                up_load(kb, s).wait()
            for s in group:
                for n0, nw in chunks:
                    v = dot(xg[s], wu[s, :, n0:n0 + nw])
                    for n in range(0, nw, LANES):
                        q = s * n_mid + (n0 + n) // LANES
                        part = acc[q, :d_mid, :] + v[:, n:n + LANES]
                        if last:
                            h_buf[s, :, n0 + n:n0 + n + LANES] = gelu(part).astype(BF16)
                        else:
                            acc[q, :d_mid, :] = part
            if not last:
                for s in group:
                    up_load(kb + 1, s).start()
            if g in after:
                after[g]()

    def up_step(kb, carry):
        def near_2():
            @pl.when(kb + 2 < n_kb)
            def _():
                stage_near(kb + 2)

            @pl.when(kb + 2 + AHEAD < n_kb)
            def _():
                start_near(kb + 2 + AHEAD)

        up_block(kb, False, {0: near_2, 1: lambda: stage_far(kb + 1)})
        return carry

    lax.fori_loop(0, n_kb - 1, up_step, 0)
    up_block(n_kb - 1, True, {})

    def mine(cb, off, h):
        return (cb * CHIPS + off) * 2 + h

    def staged(cb, off, h):
        return n_cb * CHIPS * 2 + ((cb % STAGES) * CHIPS + off) * 2 + h

    tok = pl.ds(0, n_tok)

    def to_sib(cb, off):
        return rcopy(acc.at[pl.ds(staged(cb, off, 0), 2), tok], sib_in.at[cb, off], ps_ss.at[cb, off], ps_rs.at[cb, off], sib)

    def to_far(cb):
        return (rcopy(acc.at[mine(cb, 2, 0), tok], far_in.at[cb, 0], pf_ss.at[cb, 0], pf_rs.at[cb, 0], right),
                rcopy(acc.at[mine(cb, 2, 1), tok], far_in.at[cb, 1], pf_ss.at[cb, 1], pf_rs.at[cb, 1], left))

    def to_dir(cb):
        return (rcopy(acc.at[mine(cb, 1, 1), tok], dir_in.at[cb, 0], pd_ss.at[cb, 0], pd_rs.at[cb, 0], right),
                rcopy(acc.at[mine(cb, 3, 0), tok], dir_in.at[cb, 1], pd_ss.at[cb, 1], pd_rs.at[cb, 1], left))

    def to_mrg(cb):
        return (rcopy(far_in.at[cb, 0], mrg_in.at[cb, 0], pm_ss.at[cb, 0], pm_rs.at[cb, 0], right),
                rcopy(far_in.at[cb, 1], mrg_in.at[cb, 1], pm_ss.at[cb, 1], pm_rs.at[cb, 1], left))

    def merge(cb):
        for h, off in ((0, 1), (1, prev)):
            to_far(cb)[h].wait_recv()
            far_in[cb, h] = far_in[cb, h] + acc[mine(cb, off, h), :n_tok, :]
            to_mrg(cb)[h].start()

    def finish(cb):
        for h in range(2):
            to_mrg(cb)[h].wait_recv()
            to_dir(cb)[1 - h].wait_recv()
            out = acc[mine(cb, 0, h), :n_tok, :] + mrg_in[cb, h] + dir_in[cb, 1 - h]
            y_ref[:, pl.ds(pl.multiple_of(cb * cb_w + h * LANES, LANES), LANES)] = out.astype(BF16)

    def combine(j, q):
        v = dot(c_buf[j], o_buf[j])
        v = (v[2 * n_tok:] + v[n_tok:2 * n_tok]) + v[:n_tok]
        for h in range(2):
            acc[q + h, :n_tok, :] = v[:, h * LANES:(h + 1) * LANES]

    def down_step(cb, carry):
        for group in groups:
            for s in group:
                down_load(cb, s).wait()
            for s in group:
                out = dot(h_buf[s], wd[s])
                main = out[:d_main].astype(BF16)
                for j in range(n_dev):
                    o_buf[j, s * cap:(s + 1) * cap, :] = main[j * cap:(j + 1) * cap]
                for n in range(odd):
                    first = d_main + n * n_dev
                    for h in range(cb_w // LANES):
                        o_odd[n, h, pl.ds(s, n_dev, stride=rows_s), :] = out[first:first + n_dev, h * LANES:(h + 1) * LANES]

            @pl.when(cb + 1 < n_cb)
            def _():
                for s in group:
                    down_load(cb + 1, s).start()

        for n in range(odd):
            first = rows_main + n * rows_s
            for h in range(cb_w // LANES):
                for j in range(n_dev):
                    o_buf[j, first:first + rows_s, h * LANES:(h + 1) * LANES] = o_odd[n, h, j * rows_s:(j + 1) * rows_s, :].astype(BF16)

        @pl.when(cb >= STAGES)
        def _():
            for off in range(CHIPS):
                to_sib(cb - STAGES, off).wait_send()

        order = (2, 1, prev, 0)
        for off in order:
            combine(2 * off + 1, staged(cb, off, 0))
            to_sib(cb, off).start()
        for off in order:
            combine(2 * off, mine(cb, off, 0))

        @pl.when(cb >= LAG)
        def _():
            finish(cb - LAG)

        for off in order:
            to_sib(cb, off).wait_recv()
            for h in range(2):
                q = mine(cb, off, h)
                acc[q, :n_tok, :] = acc[q, :n_tok, :] + sib_in[cb, off, h]
            if off == 2:
                for c in to_far(cb):
                    c.start()
            elif off:
                to_dir(cb)[0 if off == 1 else 1].start()

        @pl.when(cb >= 1)
        def _():
            merge(cb - 1)
        return carry

    lax.fori_loop(0, n_cb, down_step, 0)
    merge(n_cb - 1)
    for cb in range(max(0, n_cb - LAG), n_cb):
        finish(cb)

    for m in metas:
        m.wait_send()

    def drain(kb, carry):
        for c in near(kb) + relay(kb) + tuple(across(kb, off) for off in range(CHIPS)):
            c.wait_send()
        return carry

    lax.fori_loop(0, n_kb, drain, 0)

    def drain_sums(cb, carry):
        for c in to_far(cb) + to_dir(cb) + to_mrg(cb):
            c.wait_send()
        return carry

    lax.fori_loop(0, n_cb, drain_sums, 0)
    for cb in range(max(0, n_cb - STAGES), n_cb):
        for off in range(CHIPS):
            to_sib(cb, off).wait_send()


def solution(mesh):
    assert mesh.shape["ep"] == 2 * CHIPS

    def group_layer(tokens, topk_idx, topk_w, w_up, w_down, slot_expert):
        n_tok, d_model = tokens.shape
        n_top = topk_idx.shape[1]
        n_dev, n_slot = slot_expert.shape
        d_ff = w_up.shape[-1]
        bound = slot_bound(n_tok, n_top, n_dev, n_slot)
        cap = bound // 8 * 8
        odd, rows_s = bound - cap, round_up(n_slot, 16)
        kb_w, cb_w = 2 * LANES, 2 * LANES
        n_kb, n_cb = d_model // kb_w, d_model // cb_w
        d_mid = n_dev * bound
        rows_src = n_slot * cap + odd * rows_s
        n_acc = max(n_slot * (d_ff // LANES), (n_cb + STAGES) * CHIPS * 2)
        cfg = dict(bound=bound, cap=cap, kb_w=kb_w, cb_w=cb_w)
        dma = pltpu.SemaphoreType.DMA
        vmem = pl.BlockSpec(memory_space=pltpu.VMEM)
        hbm = pl.BlockSpec(memory_space=pl.ANY)
        return pl.pallas_call(
            functools.partial(moe_kernel, cfg),
            out_shape=jax.ShapeDtypeStruct((n_tok, d_model), BF16),
            in_specs=[vmem, vmem, vmem, vmem, hbm, hbm],
            out_specs=vmem,
            scratch_shapes=[
                pltpu.VMEM((n_dev, n_kb, n_tok, kb_w), BF16),
                pltpu.VMEM((n_dev, n_top, n_tok), jnp.int32),
                pltpu.VMEM((n_dev, n_top, n_tok), F32),
                pltpu.VMEM((n_slot * cap, LANES), F32),
                pltpu.VMEM((n_dev, rows_src, n_tok), BF16),
                pltpu.VMEM((n_dev, 3 * n_tok, rows_src), BF16),
                pltpu.VMEM((n_slot, d_mid, kb_w), BF16),
                pltpu.VMEM((odd, kb_w // LANES, rows_s * n_dev, LANES), F32),
                pltpu.VMEM((n_acc, max(d_mid, n_tok), LANES), F32),
                pltpu.VMEM((n_slot, d_mid, d_ff), BF16),
                pltpu.VMEM((n_dev, rows_src, cb_w), BF16),
                pltpu.VMEM((odd, cb_w // LANES, n_dev * rows_s, LANES), F32),
                pltpu.VMEM((n_slot, kb_w, d_ff), BF16),
                pltpu.VMEM((n_slot, d_ff, cb_w), BF16),
                pltpu.VMEM((n_cb, CHIPS, 2, n_tok, LANES), F32),
                pltpu.VMEM((n_cb, 2, n_tok, LANES), F32),
                pltpu.VMEM((n_cb, 2, n_tok, LANES), F32),
                pltpu.VMEM((n_cb, 2, n_tok, LANES), F32),
                dma((n_dev - 1, 2)), dma((n_dev - 1, 2)),
                dma((n_kb, 2)), dma((n_kb, 2)), dma((n_kb, 2)), dma((n_kb, 2)),
                dma((n_kb, CHIPS)), dma((n_kb, CHIPS)),
                dma((n_slot,)), dma((n_slot,)),
                dma((n_cb, CHIPS)), dma((n_cb, CHIPS)),
                dma((n_cb, 2)), dma((n_cb, 2)), dma((n_cb, 2)), dma((n_cb, 2)), dma((n_cb, 2)), dma((n_cb, 2)),
            ],
            compiler_params=pltpu.CompilerParams(collective_id=0, has_side_effects=True, vmem_limit_bytes=67_000_000),
        )(tokens, topk_idx.T, topk_w.T, slot_expert, w_up, w_down)

    row_spec = P(('dp', 'ep'), None)
    weight_spec = P('ep', None, None, None)
    return jax.shard_map(group_layer, mesh=mesh, in_specs=(row_spec, row_spec, row_spec, weight_spec, weight_spec, P(None, None)),
                         out_specs=row_spec, check_vma=False)
```

```python
import functools

import jax
import jax.numpy as jnp
from jax import lax
from jax.experimental import pallas as pl
from jax.experimental.pallas import tpu as pltpu
from jax.sharding import PartitionSpec as P

MESH = pl.DeviceIdType.MESH
F32 = jnp.float32
BF16 = jnp.bfloat16
LANES = 128
CHIPS = 4
AHEAD = 3
STAGES = 4
GROUP = 3
LAG = 3


def slot_bound(n_tok, n_top, n_dev, n_slot):
    base_load = (n_tok * n_top) // (n_dev * n_slot)
    return base_load + base_load // 2 + 1


def round_up(n, m):
    return -(-n // m) * m


def gelu(v):
    return v * (0.5 + 0.5 * jnp.tanh(v * (0.7978845608028654 + (0.7978845608028654 * 0.044715) * (v * v))))


def dot(a, b):
    return lax.dot_general(a, b, (((1,), (0,)), ((), ())), preferred_element_type=F32)


def moe_kernel(cfg, x_ref, idx_ref, gate_ref, tab_ref, wup_ref, wdn_ref, y_ref,
               xall, idx_all, gate_all, tab, trk, g_buf, c_buf, xg, xg_odd, acc, h_buf, o_buf, o_odd, wu, wd, sib_in, far_in, sum_in, y_buf,
               in_s, meta_ss, meta_rs, out_ss, near_rs, rel_rs, sib_rs, wu_s, wd_s, ps_ss, ps_rs, pf_rs, fin_rs, y_s):
    bound, cap, kb_w, cb_w = (cfg[k] for k in ("bound", "cap", "kb_w", "cb_w"))
    odd = bound - cap
    n_tok, d_model = x_ref.shape
    n_top = idx_ref.shape[0]
    n_dev, n_slot = tab_ref.shape
    d_ff = wup_ref.shape[-1]
    d_main, d_mid = n_dev * cap, n_dev * bound
    rows_s = round_up(n_slot, 16)
    rows_main, rows_src = n_slot * cap, n_slot * cap + odd * rows_s
    n_kb, n_cb = d_model // kb_w, d_model // cb_w
    half = n_tok // 2
    me = lax.axis_index("ep")
    chip, core = me // 2, me % 2

    def dev(d_chip, d_core=0):
        return {"ep": ((chip + d_chip) % CHIPS) * 2 + (core + d_core) % 2}

    right, left, sib = dev(1), dev(CHIPS - 1), dev(0, 1)

    def rcopy(src, dst, ss, rs, to):
        return pltpu.make_async_remote_copy(src_ref=src, dst_ref=dst, send_sem=ss, recv_sem=rs, device_id=to, device_id_type=MESH)

    def took(ref, sem):
        rcopy(ref, ref, sem, sem, sib).wait_send()

    def arrived(ref, sem):
        rcopy(ref, ref, sem, sem, sib).wait_recv()

    groups = [(s, min(GROUP, n_slot - s)) for s in range(0, n_slot, GROUP)]

    def up_load(kb, g):
        s, n = groups[g]
        return pltpu.make_async_copy(
            wup_ref.at[0, pl.ds(s, n), pl.ds(pl.multiple_of(kb * kb_w, kb_w), kb_w), :], wu.at[pl.ds(s, n)], wu_s.at[g])

    def down_load(cb, g):
        s, n = groups[g]
        return pltpu.make_async_copy(
            wdn_ref.at[0, pl.ds(s, n), :, pl.ds(pl.multiple_of(cb * cb_w, cb_w), cb_w)], wd.at[pl.ds(s, n)], wd_s.at[g])

    barrier = pltpu.get_barrier_semaphore()
    peers = [(dx, dc) for dx in range(CHIPS) for dc in range(2) if dx or dc]
    for dx, dc in peers:
        pl.semaphore_signal(barrier, inc=1, device_id=dev(dx, dc), device_id_type=MESH)
    in_meta = [pltpu.make_async_copy(idx_ref, idx_all.at[0], in_s.at[1]), pltpu.make_async_copy(gate_ref, gate_all.at[0], in_s.at[2]),
               pltpu.make_async_copy(tab_ref, tab, in_s.at[3])]
    for c in in_meta:
        c.start()
    for kb in range(n_kb):
        pltpu.make_async_copy(x_ref.at[:, pl.ds(kb * kb_w, kb_w)], xall.at[0, kb], in_s.at[0]).start()
    for g in range(len(groups)):
        up_load(0, g).start()
    for c in in_meta:
        c.wait()
    arrived(xall.at[0], in_s.at[0])
    pl.semaphore_wait(barrier, len(peers))

    lo, hi = pl.ds(0, half), pl.ds(half, n_tok - half)
    prev = CHIPS - 1

    def near(kb):
        return (rcopy(xall.at[0, kb], xall.at[2 * prev, kb], out_ss.at[0], near_rs.at[kb], right),
                rcopy(xall.at[0, kb], xall.at[2, kb], out_ss.at[0], near_rs.at[kb], left))

    def relay(kb):
        return (rcopy(xall.at[2 * prev, kb, lo], xall.at[4, kb, lo], out_ss.at[1], rel_rs.at[kb], right),
                rcopy(xall.at[2, kb, hi], xall.at[4, kb, hi], out_ss.at[1], rel_rs.at[kb], left))

    def across(kb, off):
        return rcopy(xall.at[2 * off, kb], xall.at[2 * off + 1, kb], out_ss.at[2], sib_rs.at[kb], sib)

    def start_near(kb):
        for c in near(kb):
            c.start()

    def stage_near(kb):
        arrived(xall.at[pl.ds(0, 2), kb], near_rs.at[kb])
        for c in relay(kb):
            c.start()
        for off in (prev, 1):
            across(kb, off).start()

    def stage_far(kb):
        arrived(xall.at[4, kb], rel_rs.at[kb])
        across(kb, 2).start()

    for dx, dc in peers:
        place = 2 * ((CHIPS - dx) % CHIPS) + dc
        rcopy(idx_all.at[0], idx_all.at[place], meta_ss.at[0], meta_rs.at[0], dev(dx, dc)).start()
        rcopy(gate_all.at[0], gate_all.at[place], meta_ss.at[1], meta_rs.at[1], dev(dx, dc)).start()
    for kb in range(AHEAD):
        start_near(kb)
    for kb in range(n_kb):
        across(kb, 0).start()
    for g in range(len(groups)):
        down_load(0, g).start()

    sub = lax.broadcasted_iota(jnp.int32, (rows_s, n_slot), 0)
    lane = lax.broadcasted_iota(jnp.int32, (rows_s, n_slot), 1)
    my_row = tab[pl.ds(me, 1), :].astype(F32)
    e_col = jnp.sum(jnp.where(sub == lane, my_row, 0.0), axis=1, keepdims=True)
    e_col = jnp.where(sub[:, 0:1] < n_slot, e_col, -2.0)
    total = jnp.zeros((rows_s, n_slot), F32)
    before = jnp.zeros((rows_s, n_slot), F32)
    for d in range(n_dev):
        same = jnp.where(tab[d:d + 1, :].astype(F32) == e_col, 1.0, 0.0)
        total = total + same
        before = before + same * jnp.where(d < me, 1.0, 0.0)
    copies = jnp.sum(total, axis=1, keepdims=True)
    my_rank = jnp.sum(before, axis=1, keepdims=True)
    r = lax.broadcasted_iota(jnp.int32, (cap, LANES), 0)
    for s in range(n_slot):
        want = r.astype(F32) * copies[s:s + 1, :] + my_rank[s:s + 1, :]
        trk[s * cap:(s + 1) * cap, :] = want
    o_odd[...] = jnp.zeros_like(o_odd)

    def clear(q, carry):
        acc[q] = jnp.zeros(acc.shape[1:], F32)
        return carry

    lax.fori_loop(0, acc.shape[0], clear, 0)
    others = pl.ds(1, n_dev - 1)
    arrived(idx_all.at[others], meta_rs.at[0])
    arrived(gate_all.at[others], meta_rs.at[1])
    lane_tok = n_tok
    earlier = (lax.broadcasted_iota(jnp.int32, (lane_tok, lane_tok), 0)
               < lax.broadcasted_iota(jnp.int32, (lane_tok, lane_tok), 1)).astype(F32).astype(BF16)
    rows_pad = round_up(rows_src, LANES)

    def route(j, carry):
        idx = idx_all[j].astype(F32)
        gates = gate_all[j]
        has = jnp.zeros((rows_s, lane_tok), F32)
        gate = jnp.zeros((rows_s, lane_tok), F32)
        for q in range(n_top):
            hit = idx[q:q + 1, :] == e_col
            has = jnp.where(hit, 1.0, has)
            gate = jnp.where(hit, gates[q:q + 1, :], gate)
        rank = jnp.where(has > 0.0, dot(has.astype(BF16), earlier), -1.0)
        parts = []
        for s in range(n_slot):
            hit = rank[s:s + 1, :] == trk[s * cap:(s + 1) * cap, 0:1]
            g_buf[j, s * cap:(s + 1) * cap, :] = jnp.where(hit, 1.0, 0.0).astype(BF16)
            parts.append(jnp.where(hit, gate[s:s + 1, :], 0.0))
        for n in range(odd):
            hit = rank == float(cap + n) * copies + my_rank
            first = rows_main + n * rows_s
            g_buf[j, first:first + rows_s, :] = jnp.where(hit, 1.0, 0.0).astype(BF16)
            parts.append(jnp.where(hit, gate, 0.0))
        if rows_pad > rows_src:
            parts.append(jnp.zeros((rows_pad - rows_src, lane_tok), F32))
        left_over = jnp.transpose(jnp.concatenate(parts, axis=0))[:, :rows_src]
        for n in range(3):
            term = left_over.astype(BF16)
            c_buf[j, n * n_tok:(n + 1) * n_tok, :] = term
            left_over = left_over - term.astype(F32)
        return carry

    lax.fori_loop(0, n_dev, route, 0)
    stage_near(0)
    start_near(AHEAD)
    stage_near(1)
    start_near(AHEAD + 1)
    stage_far(0)

    chunks = [(n, min(2 * LANES, d_ff - n)) for n in range(0, d_ff, 2 * LANES)]
    n_mid = d_ff // LANES

    def up_block(kb, last, after):
        arrived(xall.at[pl.ds(0, CHIPS), kb], sib_rs.at[kb])

        for j in range(n_dev):
            rows = dot(g_buf[j], xall[j, kb])
            main = rows[:rows_main].astype(BF16)
            for s in range(n_slot):
                xg[s, j * cap:(j + 1) * cap, :] = main[s * cap:(s + 1) * cap]
            for n in range(odd):
                first = rows_main + n * rows_s
                for h in range(kb_w // LANES):
                    xg_odd[n, h, pl.ds(j, rows_s, stride=n_dev), :] = rows[first:first + rows_s, h * LANES:(h + 1) * LANES]
        for n in range(odd):
            for h in range(kb_w // LANES):
                for s in range(n_slot):
                    xg[s, d_main + n * n_dev:d_main + (n + 1) * n_dev, h * LANES:(h + 1) * LANES] = (
                        xg_odd[n, h, s * n_dev:(s + 1) * n_dev, :].astype(BF16))
        if last:
            for g in range(len(groups)):
                up_load(kb, g).wait()
        for g, (s0, n_s) in enumerate(groups):
            if not last:
                up_load(kb, g).wait()
            for s in range(s0, s0 + n_s):
                for n0, nw in chunks:
                    v = dot(xg[s], wu[s, :, n0:n0 + nw])
                    for n in range(0, nw, LANES):
                        q = s * n_mid + (n0 + n) // LANES
                        part = acc[q, :d_mid, :] + v[:, n:n + LANES]
                        if last:
                            h_buf[s, :, n0 + n:n0 + n + LANES] = gelu(part).astype(BF16)
                        else:
                            acc[q, :d_mid, :] = part
            if not last:
                up_load(kb + 1, g).start()
            if g in after:
                after[g]()

    def up_step(kb, carry):
        def near_2():
            @pl.when(kb + 2 < n_kb)
            def _():
                stage_near(kb + 2)

            @pl.when(kb + 2 + AHEAD < n_kb)
            def _():
                start_near(kb + 2 + AHEAD)

        up_block(kb, False, {0: near_2, 1: lambda: stage_far(kb + 1)})
        return carry

    lax.fori_loop(0, n_kb - 1, up_step, 0)
    up_block(n_kb - 1, True, {})

    def mine(cb, off, h):
        return (cb * CHIPS + off) * 2 + h

    def staged(cb, off, h):
        return n_cb * CHIPS * 2 + ((cb % STAGES) * CHIPS + off) * 2 + h

    tok = pl.ds(0, n_tok)

    lots = {2: 0, 1: 1, prev: 1, 0: 2}

    def to_sib(cb, off):
        return rcopy(acc.at[pl.ds(staged(cb, off, 0), 2), tok], sib_in.at[cb, off], ps_ss.at[cb % STAGES], ps_rs.at[cb % 2, lots[off]], sib)

    def to_far(cb):
        return (rcopy(acc.at[mine(cb, 2, 0), tok], far_in.at[cb, 0], out_ss.at[3], pf_rs.at[cb], right),
                rcopy(acc.at[mine(cb, 2, 1), tok], far_in.at[cb, 1], out_ss.at[3], pf_rs.at[cb], left))

    def to_dir(cb):
        return (rcopy(acc.at[mine(cb, 1, 1), tok], sum_in.at[cb, 2], out_ss.at[4], fin_rs.at[cb], right),
                rcopy(acc.at[mine(cb, prev, 0), tok], sum_in.at[cb, 3], out_ss.at[4], fin_rs.at[cb], left))

    def to_mrg(cb):
        return (rcopy(far_in.at[cb, 0], sum_in.at[cb, 0], out_ss.at[5], fin_rs.at[cb], right),
                rcopy(far_in.at[cb, 1], sum_in.at[cb, 1], out_ss.at[5], fin_rs.at[cb], left))

    def merge(cb):
        arrived(far_in.at[cb], pf_rs.at[cb])
        for h, off in ((0, 1), (1, prev)):
            far_in[cb, h] = far_in[cb, h] + acc[mine(cb, off, h), :n_tok, :]
            to_mrg(cb)[h].start()

    def y_copy(cb):
        columns = pl.ds(pl.multiple_of(cb * cb_w, cb_w), cb_w)
        return pltpu.make_async_copy(y_buf.at[cb], y_ref.at[:, columns], y_s.at[cb])

    def finish(cb):
        arrived(sum_in.at[cb], fin_rs.at[cb])
        for h in range(2):
            out = acc[mine(cb, 0, h), :n_tok, :] + sum_in[cb, h] + sum_in[cb, 3 - h]
            y_buf[cb, :, h * LANES:(h + 1) * LANES] = out.astype(BF16)
        y_copy(cb).start()

    def add_sib(cb, off):
        for h in range(2):
            q = mine(cb, off, h)
            acc[q, :n_tok, :] = acc[q, :n_tok, :] + sib_in[cb, off, h]

    def combine(j, q):
        v = dot(c_buf[j], o_buf[j])
        v = (v[2 * n_tok:] + v[n_tok:2 * n_tok]) + v[:n_tok]
        for h in range(2):
            acc[q + h, :n_tok, :] = v[:, h * LANES:(h + 1) * LANES]

    def down_step(cb, carry):
        for g, (s0, n_s) in enumerate(groups):
            down_load(cb, g).wait()
            for s in range(s0, s0 + n_s):
                out = dot(h_buf[s], wd[s])
                main = out[:d_main].astype(BF16)
                for j in range(n_dev):
                    o_buf[j, s * cap:(s + 1) * cap, :] = main[j * cap:(j + 1) * cap]
                for n in range(odd):
                    first = d_main + n * n_dev
                    for h in range(cb_w // LANES):
                        o_odd[n, h, pl.ds(s, n_dev, stride=rows_s), :] = out[first:first + n_dev, h * LANES:(h + 1) * LANES]

            @pl.when(cb + 1 < n_cb)
            def _():
                down_load(cb + 1, g).start()

        for n in range(odd):
            first = rows_main + n * rows_s
            for h in range(cb_w // LANES):
                for j in range(n_dev):
                    o_buf[j, first:first + rows_s, h * LANES:(h + 1) * LANES] = o_odd[n, h, j * rows_s:(j + 1) * rows_s, :].astype(BF16)

        @pl.when(cb >= STAGES)
        def _():
            took(acc.at[pl.ds(staged(cb, 0, 0), 2 * CHIPS), tok], ps_ss.at[cb % STAGES])

        def for_sib(off):
            combine(2 * off + 1, staged(cb, off, 0))
            to_sib(cb, off).start()

        for off in (2, 1, prev):
            for_sib(off)
        combine(2 * 2, mine(cb, 2, 0))
        arrived(sib_in.at[cb, 2], ps_rs.at[cb % 2, 0])
        add_sib(cb, 2)
        for c in to_far(cb):
            c.start()
        for_sib(0)
        for off in (1, prev):
            combine(2 * off, mine(cb, off, 0))
        arrived(sib_in.at[cb, pl.ds(0, 2)], ps_rs.at[cb % 2, 1])
        for n, off in enumerate((1, prev)):
            add_sib(cb, off)
            to_dir(cb)[n].start()
        combine(0, mine(cb, 0, 0))

        @pl.when(cb >= LAG)
        def _():
            finish(cb - LAG)

        arrived(sib_in.at[cb, 0], ps_rs.at[cb % 2, 2])
        add_sib(cb, 0)

        @pl.when(cb >= 1)
        def _():
            merge(cb - 1)
        return carry

    lax.fori_loop(0, n_cb, down_step, 0)
    merge(n_cb - 1)
    for cb in range(max(0, n_cb - LAG), n_cb):
        finish(cb)

    took(idx_all.at[others], meta_ss.at[0])
    took(gate_all.at[others], meta_ss.at[1])
    for n, ref in enumerate((xall.at[pl.ds(0, 2)], xall.at[4], xall.at[pl.ds(0, CHIPS)], far_in, far_in, far_in)):
        took(ref, out_ss.at[n])
    for n in range(min(STAGES, n_cb)):
        took(acc.at[pl.ds(staged(n, 0, 0), 2 * CHIPS), tok], ps_ss.at[n])
    for cb in range(n_cb):
        y_copy(cb).wait()


def solution(mesh):
    assert mesh.shape["ep"] == 2 * CHIPS

    def group_layer(tokens, topk_idx, topk_w, w_up, w_down, slot_expert):
        n_tok, d_model = tokens.shape
        n_top = topk_idx.shape[1]
        n_dev, n_slot = slot_expert.shape
        d_ff = w_up.shape[-1]
        bound = slot_bound(n_tok, n_top, n_dev, n_slot)
        cap = bound // 8 * 8
        odd, rows_s = bound - cap, round_up(n_slot, 16)
        kb_w, cb_w = 2 * LANES, 2 * LANES
        n_kb, n_cb = d_model // kb_w, d_model // cb_w
        d_mid = n_dev * bound
        rows_src = n_slot * cap + odd * rows_s
        n_acc = max(n_slot * (d_ff // LANES), (n_cb + STAGES) * CHIPS * 2)
        cfg = dict(bound=bound, cap=cap, kb_w=kb_w, cb_w=cb_w)
        dma = pltpu.SemaphoreType.DMA
        hbm = pl.BlockSpec(memory_space=pl.ANY)
        return pl.pallas_call(
            functools.partial(moe_kernel, cfg),
            out_shape=jax.ShapeDtypeStruct((n_tok, d_model), BF16),
            in_specs=[hbm] * 6,
            out_specs=hbm,
            scratch_shapes=[
                pltpu.VMEM((n_dev, n_kb, n_tok, kb_w), BF16),
                pltpu.VMEM((n_dev, n_top, n_tok), jnp.int32),
                pltpu.VMEM((n_dev, n_top, n_tok), F32),
                pltpu.VMEM((n_dev, n_slot), jnp.int32),
                pltpu.VMEM((n_slot * cap, LANES), F32),
                pltpu.VMEM((n_dev, rows_src, n_tok), BF16),
                pltpu.VMEM((n_dev, 3 * n_tok, rows_src), BF16),
                pltpu.VMEM((n_slot, d_mid, kb_w), BF16),
                pltpu.VMEM((odd, kb_w // LANES, rows_s * n_dev, LANES), F32),
                pltpu.VMEM((n_acc, max(d_mid, n_tok), LANES), F32),
                pltpu.VMEM((n_slot, d_mid, d_ff), BF16),
                pltpu.VMEM((n_dev, rows_src, cb_w), BF16),
                pltpu.VMEM((odd, cb_w // LANES, n_dev * rows_s, LANES), F32),
                pltpu.VMEM((n_slot, kb_w, d_ff), BF16),
                pltpu.VMEM((n_slot, d_ff, cb_w), BF16),
                pltpu.VMEM((n_cb, CHIPS, 2, n_tok, LANES), F32),
                pltpu.VMEM((n_cb, 2, n_tok, LANES), F32),
                pltpu.VMEM((n_cb, 4, n_tok, LANES), F32),
                pltpu.VMEM((n_cb, n_tok, cb_w), BF16),
                dma((4,)), dma((2,)), dma((2,)), dma((6,)),
                dma((n_kb,)), dma((n_kb,)), dma((n_kb,)),
                dma((-(-n_slot // GROUP),)), dma((-(-n_slot // GROUP),)),
                dma((STAGES,)), dma((2, 3)), dma((n_cb,)), dma((n_cb,)), dma((n_cb,)),
            ],
            compiler_params=pltpu.CompilerParams(collective_id=0, has_side_effects=True, vmem_limit_bytes=67_000_000),
        )(tokens, topk_idx.T, topk_w.T, slot_expert, w_up, w_down)

    row_spec = P(('dp', 'ep'), None)
    weight_spec = P('ep', None, None, None)
    return jax.shard_map(group_layer, mesh=mesh, in_specs=(row_spec, row_spec, row_spec, weight_spec, weight_spec, P(None, None)),
                         out_specs=row_spec, check_vma=False)
```

```python
import functools

import jax
import jax.numpy as jnp
from jax import lax
from jax.experimental import pallas as pl
from jax.experimental.pallas import tpu as pltpu
from jax.sharding import PartitionSpec as P

MESH = pl.DeviceIdType.MESH
F32 = jnp.float32
BF16 = jnp.bfloat16
LANES = 128
CHIPS = 4
AHEAD = 3
STAGES = 4
GROUP = 3
LAG = 3


def slot_bound(n_tok, n_top, n_dev, n_slot):
    base_load = (n_tok * n_top) // (n_dev * n_slot)
    return base_load + base_load // 2 + 1


def round_up(n, m):
    return -(-n // m) * m


def gelu(v):
    return v * (0.5 + 0.5 * jnp.tanh(v * (0.7978845608028654 + (0.7978845608028654 * 0.044715) * (v * v))))


def dot(a, b):
    return lax.dot_general(a, b, (((1,), (0,)), ((), ())), preferred_element_type=F32)


def moe_kernel(cfg, x_ref, idx_ref, gate_ref, tab_ref, wup_ref, wdn_ref, y_ref,
               xall, idx_all, gate_all, tab, trk, g_buf, c_buf, xg, xg_odd, acc, h_buf, o_buf, o_odd, wu, wd, sib_in, far_in, sum_in, y_buf,
               in_s, meta_ss, meta_rs, out_ss, near_rs, rel_rs, sib_rs, wu_s, wd_s, ps_ss, ps_rs, pf_rs, fin_rs, y_s):
    bound, cap, kb_w, cb_w = (cfg[k] for k in ("bound", "cap", "kb_w", "cb_w"))
    odd = bound - cap
    n_tok, d_model = x_ref.shape
    n_top = idx_ref.shape[0]
    n_dev, n_slot = tab_ref.shape
    d_ff = wup_ref.shape[-1]
    d_main, d_mid = n_dev * cap, n_dev * bound
    rows_s = round_up(n_slot, 16)
    rows_main, rows_src = n_slot * cap, n_slot * cap + odd * rows_s
    n_kb, n_cb = d_model // kb_w, d_model // cb_w
    half = n_tok // 2
    me = lax.axis_index("ep")
    chip, core = me // 2, me % 2

    def dev(d_chip, d_core=0):
        return {"ep": ((chip + d_chip) % CHIPS) * 2 + (core + d_core) % 2}

    right, left, sib = dev(1), dev(CHIPS - 1), dev(0, 1)

    def rcopy(src, dst, ss, rs, to):
        return pltpu.make_async_remote_copy(src_ref=src, dst_ref=dst, send_sem=ss, recv_sem=rs, device_id=to, device_id_type=MESH)

    def took(ref, sem):
        rcopy(ref, ref, sem, sem, sib).wait_send()

    def arrived(ref, sem):
        rcopy(ref, ref, sem, sem, sib).wait_recv()

    groups = [(s, min(GROUP, n_slot - s)) for s in range(0, n_slot, GROUP)]

    class Loads:
        def __init__(self, src, dst, sem, g):
            (s, n), self.src, self.dst, self.sem = groups[g], src, dst, sem.at[g]
            self.slots, self.all = range(s, s + n), pl.ds(s, n)

        def start(self):
            for s in self.slots:
                pltpu.make_async_copy(self.src(s), self.dst.at[s], self.sem).start()

        def wait(self):
            pltpu.make_async_copy(self.src(self.all), self.dst.at[self.all], self.sem).wait()

    def up_load(kb, g):
        return Loads(lambda s: wup_ref.at[0, s, pl.ds(pl.multiple_of(kb * kb_w, kb_w), kb_w), :], wu, wu_s, g)

    def down_load(cb, g):
        return Loads(lambda s: wdn_ref.at[0, s, :, pl.ds(pl.multiple_of(cb * cb_w, cb_w), cb_w)], wd, wd_s, g)

    barrier = pltpu.get_barrier_semaphore()
    peers = [(dx, dc) for dx in range(CHIPS) for dc in range(2) if dx or dc]
    for dx, dc in peers:
        pl.semaphore_signal(barrier, inc=1, device_id=dev(dx, dc), device_id_type=MESH)
    in_meta = [pltpu.make_async_copy(idx_ref, idx_all.at[0], in_s.at[1]), pltpu.make_async_copy(gate_ref, gate_all.at[0], in_s.at[2]),
               pltpu.make_async_copy(tab_ref, tab, in_s.at[3])]
    for c in in_meta:
        c.start()
    for kb in range(n_kb):
        pltpu.make_async_copy(x_ref.at[:, pl.ds(kb * kb_w, kb_w)], xall.at[0, kb], in_s.at[0]).start()
    for g in range(len(groups)):
        up_load(0, g).start()
    for c in in_meta:
        c.wait()
    with jax.named_scope("inputs"):
        arrived(xall.at[0], in_s.at[0])
    with jax.named_scope("barrier"):
        pl.semaphore_wait(barrier, len(peers))

    lo, hi = pl.ds(0, half), pl.ds(half, n_tok - half)
    prev = CHIPS - 1

    def near(kb):
        return (rcopy(xall.at[0, kb], xall.at[2 * prev, kb], out_ss.at[0], near_rs.at[kb], right),
                rcopy(xall.at[0, kb], xall.at[2, kb], out_ss.at[0], near_rs.at[kb], left))

    def relay(kb):
        return (rcopy(xall.at[2 * prev, kb, lo], xall.at[4, kb, lo], out_ss.at[1], rel_rs.at[kb], right),
                rcopy(xall.at[2, kb, hi], xall.at[4, kb, hi], out_ss.at[1], rel_rs.at[kb], left))

    def across(kb, off):
        return rcopy(xall.at[2 * off, kb], xall.at[2 * off + 1, kb], out_ss.at[2], sib_rs.at[kb], sib)

    def start_near(kb):
        for c in near(kb):
            c.start()

    def stage_near(kb):
        arrived(xall.at[pl.ds(0, 2), kb], near_rs.at[kb])
        for c in relay(kb):
            c.start()
        for off in (prev, 1):
            across(kb, off).start()

    def stage_far(kb):
        arrived(xall.at[4, kb], rel_rs.at[kb])
        across(kb, 2).start()

    for dx, dc in peers:
        place = 2 * ((CHIPS - dx) % CHIPS) + dc
        rcopy(idx_all.at[0], idx_all.at[place], meta_ss.at[0], meta_rs.at[0], dev(dx, dc)).start()
        rcopy(gate_all.at[0], gate_all.at[place], meta_ss.at[1], meta_rs.at[1], dev(dx, dc)).start()
    for kb in range(AHEAD):
        start_near(kb)
    for kb in range(n_kb):
        across(kb, 0).start()
    for g in range(len(groups)):
        down_load(0, g).start()

    sub = lax.broadcasted_iota(jnp.int32, (rows_s, n_slot), 0)
    lane = lax.broadcasted_iota(jnp.int32, (rows_s, n_slot), 1)
    my_row = tab[pl.ds(me, 1), :].astype(F32)
    e_col = jnp.sum(jnp.where(sub == lane, my_row, 0.0), axis=1, keepdims=True)
    e_col = jnp.where(sub[:, 0:1] < n_slot, e_col, -2.0)
    total = jnp.zeros((rows_s, n_slot), F32)
    before = jnp.zeros((rows_s, n_slot), F32)
    for d in range(n_dev):
        same = jnp.where(tab[d:d + 1, :].astype(F32) == e_col, 1.0, 0.0)
        total = total + same
        before = before + same * jnp.where(d < me, 1.0, 0.0)
    copies = jnp.sum(total, axis=1, keepdims=True)
    my_rank = jnp.sum(before, axis=1, keepdims=True)
    r = lax.broadcasted_iota(jnp.int32, (cap, LANES), 0)
    for s in range(n_slot):
        want = r.astype(F32) * copies[s:s + 1, :] + my_rank[s:s + 1, :]
        trk[s * cap:(s + 1) * cap, :] = want
    o_odd[...] = jnp.zeros_like(o_odd)

    def clear(q, carry):
        acc[q] = jnp.zeros(acc.shape[1:], F32)
        return carry

    lax.fori_loop(0, acc.shape[0], clear, 0)
    others = pl.ds(1, n_dev - 1)
    with jax.named_scope("meta"):
        arrived(idx_all.at[others], meta_rs.at[0])
        arrived(gate_all.at[others], meta_rs.at[1])
    lane_tok = n_tok
    earlier = (lax.broadcasted_iota(jnp.int32, (lane_tok, lane_tok), 0)
               < lax.broadcasted_iota(jnp.int32, (lane_tok, lane_tok), 1)).astype(F32).astype(BF16)
    rows_pad = round_up(rows_src, LANES)

    def route(j, carry):
        idx = idx_all[j].astype(F32)
        gates = gate_all[j]
        has = jnp.zeros((rows_s, lane_tok), F32)
        gate = jnp.zeros((rows_s, lane_tok), F32)
        for q in range(n_top):
            hit = idx[q:q + 1, :] == e_col
            has = jnp.where(hit, 1.0, has)
            gate = jnp.where(hit, gates[q:q + 1, :], gate)
        rank = jnp.where(has > 0.0, dot(has.astype(BF16), earlier), -1.0)
        parts = []
        for s in range(n_slot):
            hit = rank[s:s + 1, :] == trk[s * cap:(s + 1) * cap, 0:1]
            g_buf[j, s * cap:(s + 1) * cap, :] = jnp.where(hit, 1.0, 0.0).astype(BF16)
            parts.append(jnp.where(hit, gate[s:s + 1, :], 0.0))
        for n in range(odd):
            hit = rank == float(cap + n) * copies + my_rank
            first = rows_main + n * rows_s
            g_buf[j, first:first + rows_s, :] = jnp.where(hit, 1.0, 0.0).astype(BF16)
            parts.append(jnp.where(hit, gate, 0.0))
        if rows_pad > rows_src:
            parts.append(jnp.zeros((rows_pad - rows_src, lane_tok), F32))
        left_over = jnp.transpose(jnp.concatenate(parts, axis=0))[:, :rows_src]
        for n in range(3):
            term = left_over.astype(BF16)
            c_buf[j, n * n_tok:(n + 1) * n_tok, :] = term
            left_over = left_over - term.astype(F32)
        return carry

    with jax.named_scope("route"):
        lax.fori_loop(0, n_dev, route, 0)
    with jax.named_scope("near0"):
        stage_near(0)
    start_near(AHEAD)
    with jax.named_scope("near1"):
        stage_near(1)
    start_near(AHEAD + 1)
    with jax.named_scope("far0"):
        stage_far(0)

    chunks = [(n, min(2 * LANES, d_ff - n)) for n in range(0, d_ff, 2 * LANES)]
    n_mid = d_ff // LANES

    def up_block(kb, last, after):
        with jax.named_scope("across"):
            arrived(xall.at[pl.ds(0, CHIPS), kb], sib_rs.at[kb])

        for j in range(n_dev):
            rows = dot(g_buf[j], xall[j, kb])
            main = rows[:rows_main].astype(BF16)
            for s in range(n_slot):
                xg[s, j * cap:(j + 1) * cap, :] = main[s * cap:(s + 1) * cap]
            for n in range(odd):
                first = rows_main + n * rows_s
                for h in range(kb_w // LANES):
                    xg_odd[n, h, pl.ds(j, rows_s, stride=n_dev), :] = rows[first:first + rows_s, h * LANES:(h + 1) * LANES]
        for n in range(odd):
            for h in range(kb_w // LANES):
                for s in range(n_slot):
                    xg[s, d_main + n * n_dev:d_main + (n + 1) * n_dev, h * LANES:(h + 1) * LANES] = (
                        xg_odd[n, h, s * n_dev:(s + 1) * n_dev, :].astype(BF16))
        with jax.named_scope("lastload"):
            if last:
                for g in range(len(groups)):
                    up_load(kb, g).wait()
        for g, (s0, n_s) in enumerate(groups):
            with jax.named_scope(f"upload{g}"):
                if not last:
                    up_load(kb, g).wait()
            for s in range(s0, s0 + n_s):
                for n0, nw in chunks:
                    v = dot(xg[s], wu[s, :, n0:n0 + nw])
                    for n in range(0, nw, LANES):
                        q = s * n_mid + (n0 + n) // LANES
                        part = acc[q, :d_mid, :] + v[:, n:n + LANES]
                        if last:
                            h_buf[s, :, n0 + n:n0 + n + LANES] = gelu(part).astype(BF16)
                        else:
                            acc[q, :d_mid, :] = part
            if not last:
                up_load(kb + 1, g).start()
            with jax.named_scope(f"stage{g}"):
                if g in after:
                    after[g]()

    def up_step(kb, carry):
        def near_2():
            @pl.when(kb + 2 < n_kb)
            def _():
                stage_near(kb + 2)

            @pl.when(kb + 2 + AHEAD < n_kb)
            def _():
                start_near(kb + 2 + AHEAD)

        up_block(kb, False, {0: near_2, 1: lambda: stage_far(kb + 1)})
        return carry

    lax.fori_loop(0, n_kb - 1, up_step, 0)
    up_block(n_kb - 1, True, {})

    def mine(cb, off, h):
        return (cb * CHIPS + off) * 2 + h

    def staged(cb, off, h):
        return n_cb * CHIPS * 2 + ((cb % STAGES) * CHIPS + off) * 2 + h

    tok = pl.ds(0, n_tok)

    lots = {2: 0, 1: 1, prev: 1, 0: 2}

    def to_sib(cb, off):
        return rcopy(acc.at[pl.ds(staged(cb, off, 0), 2), tok], sib_in.at[cb, off], ps_ss.at[cb % STAGES], ps_rs.at[cb % 2, lots[off]], sib)

    def to_far(cb):
        return (rcopy(acc.at[mine(cb, 2, 0), tok], far_in.at[cb, 0], out_ss.at[3], pf_rs.at[cb], right),
                rcopy(acc.at[mine(cb, 2, 1), tok], far_in.at[cb, 1], out_ss.at[3], pf_rs.at[cb], left))

    def to_dir(cb):
        return (rcopy(acc.at[mine(cb, 1, 1), tok], sum_in.at[cb, 2], out_ss.at[4], fin_rs.at[cb], right),
                rcopy(acc.at[mine(cb, prev, 0), tok], sum_in.at[cb, 3], out_ss.at[4], fin_rs.at[cb], left))

    def to_mrg(cb):
        return (rcopy(far_in.at[cb, 0], sum_in.at[cb, 0], out_ss.at[5], fin_rs.at[cb], right),
                rcopy(far_in.at[cb, 1], sum_in.at[cb, 1], out_ss.at[5], fin_rs.at[cb], left))

    def merge(cb):
        arrived(far_in.at[cb], pf_rs.at[cb])
        for h, off in ((0, 1), (1, prev)):
            far_in[cb, h] = far_in[cb, h] + acc[mine(cb, off, h), :n_tok, :]
            to_mrg(cb)[h].start()

    def y_copy(cb):
        columns = pl.ds(pl.multiple_of(cb * cb_w, cb_w), cb_w)
        return pltpu.make_async_copy(y_buf.at[cb], y_ref.at[:, columns], y_s.at[cb])

    def finish(cb):
        arrived(sum_in.at[cb], fin_rs.at[cb])
        for h in range(2):
            out = acc[mine(cb, 0, h), :n_tok, :] + sum_in[cb, h] + sum_in[cb, 3 - h]
            y_buf[cb, :, h * LANES:(h + 1) * LANES] = out.astype(BF16)
        y_copy(cb).start()

    def add_sib(cb, off):
        for h in range(2):
            q = mine(cb, off, h)
            acc[q, :n_tok, :] = acc[q, :n_tok, :] + sib_in[cb, off, h]

    def combine(j, q):
        v = dot(c_buf[j], o_buf[j])
        v = (v[2 * n_tok:] + v[n_tok:2 * n_tok]) + v[:n_tok]
        for h in range(2):
            acc[q + h, :n_tok, :] = v[:, h * LANES:(h + 1) * LANES]

    def down_step(cb, carry):
        for g, (s0, n_s) in enumerate(groups):
            with jax.named_scope("download"):
                down_load(cb, g).wait()
            for s in range(s0, s0 + n_s):
                out = dot(h_buf[s], wd[s])
                main = out[:d_main].astype(BF16)
                for j in range(n_dev):
                    o_buf[j, s * cap:(s + 1) * cap, :] = main[j * cap:(j + 1) * cap]
                for n in range(odd):
                    first = d_main + n * n_dev
                    for h in range(cb_w // LANES):
                        o_odd[n, h, pl.ds(s, n_dev, stride=rows_s), :] = out[first:first + n_dev, h * LANES:(h + 1) * LANES]

            @pl.when(cb + 1 < n_cb)
            def _():
                down_load(cb + 1, g).start()

        for n in range(odd):
            first = rows_main + n * rows_s
            for h in range(cb_w // LANES):
                for j in range(n_dev):
                    o_buf[j, first:first + rows_s, h * LANES:(h + 1) * LANES] = o_odd[n, h, j * rows_s:(j + 1) * rows_s, :].astype(BF16)

        @pl.when(cb >= STAGES)
        def _():
            took(acc.at[pl.ds(staged(cb, 0, 0), 2 * CHIPS), tok], ps_ss.at[cb % STAGES])

        def for_sib(off):
            combine(2 * off + 1, staged(cb, off, 0))
            to_sib(cb, off).start()

        for off in (2, 1, prev):
            for_sib(off)
        combine(2 * 2, mine(cb, 2, 0))
        with jax.named_scope("sibF"):
            arrived(sib_in.at[cb, 2], ps_rs.at[cb % 2, 0])
        add_sib(cb, 2)
        for c in to_far(cb):
            c.start()
        for_sib(0)
        for off in (1, prev):
            combine(2 * off, mine(cb, off, 0))
        with jax.named_scope("sibRL"):
            arrived(sib_in.at[cb, pl.ds(0, 2)], ps_rs.at[cb % 2, 1])
        for n, off in enumerate((1, prev)):
            add_sib(cb, off)
            to_dir(cb)[n].start()
        combine(0, mine(cb, 0, 0))

        with jax.named_scope("finish"):
            @pl.when(cb >= LAG)
            def _():
                finish(cb - LAG)

        arrived(sib_in.at[cb, 0], ps_rs.at[cb % 2, 2])
        add_sib(cb, 0)

        with jax.named_scope("merge"):
            @pl.when(cb >= 1)
            def _():
                merge(cb - 1)
        return carry

    lax.fori_loop(0, n_cb, down_step, 0)
    with jax.named_scope("merge_last"):
        merge(n_cb - 1)
    with jax.named_scope("finish_last"):
        for cb in range(max(0, n_cb - LAG), n_cb):
            finish(cb)

    took(idx_all.at[others], meta_ss.at[0])
    took(gate_all.at[others], meta_ss.at[1])
    for n, ref in enumerate((xall.at[pl.ds(0, 2)], xall.at[4], xall.at[pl.ds(0, CHIPS)], far_in, far_in, far_in)):
        took(ref, out_ss.at[n])
    for n in range(min(STAGES, n_cb)):
        took(acc.at[pl.ds(staged(n, 0, 0), 2 * CHIPS), tok], ps_ss.at[n])
    for cb in range(n_cb):
        y_copy(cb).wait()


def solution(mesh):
    assert mesh.shape["ep"] == 2 * CHIPS

    def group_layer(tokens, topk_idx, topk_w, w_up, w_down, slot_expert):
        n_tok, d_model = tokens.shape
        n_top = topk_idx.shape[1]
        n_dev, n_slot = slot_expert.shape
        d_ff = w_up.shape[-1]
        bound = slot_bound(n_tok, n_top, n_dev, n_slot)
        cap = bound // 8 * 8
        odd, rows_s = bound - cap, round_up(n_slot, 16)
        kb_w, cb_w = 2 * LANES, 2 * LANES
        n_kb, n_cb = d_model // kb_w, d_model // cb_w
        d_mid = n_dev * bound
        rows_src = n_slot * cap + odd * rows_s
        n_acc = max(n_slot * (d_ff // LANES), (n_cb + STAGES) * CHIPS * 2)
        cfg = dict(bound=bound, cap=cap, kb_w=kb_w, cb_w=cb_w)
        dma = pltpu.SemaphoreType.DMA
        hbm = pl.BlockSpec(memory_space=pl.ANY)
        return pl.pallas_call(
            functools.partial(moe_kernel, cfg),
            out_shape=jax.ShapeDtypeStruct((n_tok, d_model), BF16),
            in_specs=[hbm] * 6,
            out_specs=hbm,
            scratch_shapes=[
                pltpu.VMEM((n_dev, n_kb, n_tok, kb_w), BF16),
                pltpu.VMEM((n_dev, n_top, n_tok), jnp.int32),
                pltpu.VMEM((n_dev, n_top, n_tok), F32),
                pltpu.VMEM((n_dev, n_slot), jnp.int32),
                pltpu.VMEM((n_slot * cap, LANES), F32),
                pltpu.VMEM((n_dev, rows_src, n_tok), BF16),
                pltpu.VMEM((n_dev, 3 * n_tok, rows_src), BF16),
                pltpu.VMEM((n_slot, d_mid, kb_w), BF16),
                pltpu.VMEM((odd, kb_w // LANES, rows_s * n_dev, LANES), F32),
                pltpu.VMEM((n_acc, max(d_mid, n_tok), LANES), F32),
                pltpu.VMEM((n_slot, d_mid, d_ff), BF16),
                pltpu.VMEM((n_dev, rows_src, cb_w), BF16),
                pltpu.VMEM((odd, cb_w // LANES, n_dev * rows_s, LANES), F32),
                pltpu.VMEM((n_slot, kb_w, d_ff), BF16),
                pltpu.VMEM((n_slot, d_ff, cb_w), BF16),
                pltpu.VMEM((n_cb, CHIPS, 2, n_tok, LANES), F32),
                pltpu.VMEM((n_cb, 2, n_tok, LANES), F32),
                pltpu.VMEM((n_cb, 4, n_tok, LANES), F32),
                pltpu.VMEM((n_cb, n_tok, cb_w), BF16),
                dma((4,)), dma((2,)), dma((2,)), dma((6,)),
                dma((n_kb,)), dma((n_kb,)), dma((n_kb,)),
                dma((-(-n_slot // GROUP),)), dma((-(-n_slot // GROUP),)),
                dma((STAGES,)), dma((2, 3)), dma((n_cb,)), dma((n_cb,)), dma((n_cb,)),
            ],
            compiler_params=pltpu.CompilerParams(collective_id=0, has_side_effects=True, vmem_limit_bytes=67_000_000),
        )(tokens, topk_idx.T, topk_w.T, slot_expert, w_up, w_down)

    row_spec = P(('dp', 'ep'), None)
    weight_spec = P('ep', None, None, None)
    return jax.shard_map(group_layer, mesh=mesh, in_specs=(row_spec, row_spec, row_spec, weight_spec, weight_spec, P(None, None)),
                         out_specs=row_spec, check_vma=False)
```

```python
import functools

import jax
import jax.numpy as jnp
from jax import lax
from jax.experimental import pallas as pl
from jax.experimental.pallas import tpu as pltpu
from jax.sharding import PartitionSpec as P

MESH = pl.DeviceIdType.MESH
F32 = jnp.float32
BF16 = jnp.bfloat16
LANES = 128
CHIPS = 4
AHEAD = 2
STAGES = 4
GROUP = 3
LAG = 3


def slot_bound(n_tok, n_top, n_dev, n_slot):
    base_load = (n_tok * n_top) // (n_dev * n_slot)
    return base_load + base_load // 2 + 1


def round_up(n, m):
    return -(-n // m) * m


def gelu(v):
    return v * (0.5 + 0.5 * jnp.tanh(v * (0.7978845608028654 + (0.7978845608028654 * 0.044715) * (v * v))))


def dot(a, b):
    return lax.dot_general(a, b, (((1,), (0,)), ((), ())), preferred_element_type=F32)


def moe_kernel(cfg, x_ref, idx_ref, gate_ref, tab_ref, wup_ref, wdn_ref, y_ref,
               xall, idx_all, gate_all, rank_all, tab, trk, g_buf, c_buf, xg, xg_odd, acc, h_buf, o_buf, o_odd, wu, wd, sib_in, far_in, sum_in, y_buf,
               in_s, meta_ss, meta_rs, out_ss, near_rs, rel_rs, sib_rs, wu_s, wd_s, ps_ss, ps_rs, pf_rs, fin_rs, y_s):
    bound, cap, kb_w, cb_w = (cfg[k] for k in ("bound", "cap", "kb_w", "cb_w"))
    odd = bound - cap
    n_tok, d_model = x_ref.shape
    n_top = idx_ref.shape[0]
    n_dev, n_slot = tab_ref.shape
    d_ff = wup_ref.shape[-1]
    d_main, d_mid = n_dev * cap, n_dev * bound
    rows_s = round_up(n_slot, 16)
    rows_main, rows_src = n_slot * cap, n_slot * cap + odd * rows_s
    n_kb, n_cb = d_model // kb_w, d_model // cb_w
    half = n_tok // 2
    me = lax.axis_index("ep")
    chip, core = me // 2, me % 2

    def dev(d_chip, d_core=0):
        return {"ep": ((chip + d_chip) % CHIPS) * 2 + (core + d_core) % 2}

    right, left, sib = dev(1), dev(CHIPS - 1), dev(0, 1)

    def rcopy(src, dst, ss, rs, to):
        return pltpu.make_async_remote_copy(src_ref=src, dst_ref=dst, send_sem=ss, recv_sem=rs, device_id=to, device_id_type=MESH)

    def took(ref, sem):
        rcopy(ref, ref, sem, sem, sib).wait_send()

    def arrived(ref, sem):
        rcopy(ref, ref, sem, sem, sib).wait_recv()

    groups = [(s, min(GROUP, n_slot - s)) for s in range(0, n_slot, GROUP)]

    class Loads:
        def __init__(self, src, dst, sem, g):
            (s, n), self.src, self.dst, self.sem = groups[g], src, dst, sem.at[g]
            self.slots, self.all = range(s, s + n), pl.ds(s, n)

        def start(self):
            for s in self.slots:
                pltpu.make_async_copy(self.src(s), self.dst.at[s], self.sem).start()

        def wait(self):
            pltpu.make_async_copy(self.src(self.all), self.dst.at[self.all], self.sem).wait()

    def up_load(kb, g):
        return Loads(lambda s: wup_ref.at[0, s, pl.ds(pl.multiple_of(kb * kb_w, kb_w), kb_w), :], wu, wu_s, g)

    def down_load(cb, g):
        return Loads(lambda s: wdn_ref.at[0, s, :, pl.ds(pl.multiple_of(cb * cb_w, cb_w), cb_w)], wd, wd_s, g)

    barrier = pltpu.get_barrier_semaphore()
    peers = [(dx, dc) for dx in range(CHIPS) for dc in range(2) if dx or dc]
    for dx, dc in peers:
        pl.semaphore_signal(barrier, inc=1, device_id=dev(dx, dc), device_id_type=MESH)
    in_meta = [pltpu.make_async_copy(idx_ref, idx_all.at[0], in_s.at[1]), pltpu.make_async_copy(gate_ref, gate_all.at[0], in_s.at[2]),
               pltpu.make_async_copy(tab_ref, tab, in_s.at[3])]
    for c in in_meta:
        c.start()
    for kb in range(n_kb):
        pltpu.make_async_copy(x_ref.at[:, pl.ds(kb * kb_w, kb_w)], xall.at[0, kb], in_s.at[0]).start()
    with jax.named_scope("inputs"):
        arrived(xall.at[0], in_s.at[0])
    for c in in_meta:
        c.wait()
    with jax.named_scope("barrier"):
        pl.semaphore_wait(barrier, len(peers))

    lo, hi = pl.ds(0, half), pl.ds(half, n_tok - half)
    prev = CHIPS - 1

    def near(kb):
        return (rcopy(xall.at[0, kb], xall.at[2 * prev, kb], out_ss.at[0], near_rs.at[kb], right),
                rcopy(xall.at[0, kb], xall.at[2, kb], out_ss.at[0], near_rs.at[kb], left))

    def relay(kb):
        return (rcopy(xall.at[2 * prev, kb, lo], xall.at[4, kb, lo], out_ss.at[1], rel_rs.at[kb], right),
                rcopy(xall.at[2, kb, hi], xall.at[4, kb, hi], out_ss.at[1], rel_rs.at[kb], left))

    def across(kb, off):
        return rcopy(xall.at[2 * off, kb], xall.at[2 * off + 1, kb], out_ss.at[2], sib_rs.at[kb], sib)

    def start_near(kb):
        for c in near(kb):
            c.start()

    def stage_near(kb):
        arrived(xall.at[pl.ds(0, 2), kb], near_rs.at[kb])
        for c in relay(kb):
            c.start()
        for off in (prev, 1):
            across(kb, off).start()

    def stage_far(kb):
        arrived(xall.at[4, kb], rel_rs.at[kb])
        across(kb, 2).start()

    def send_meta(ref, n):
        for dx, dc in peers:
            place = 2 * ((CHIPS - dx) % CHIPS) + dc
            rcopy(ref.at[0], ref.at[place], meta_ss.at[n], meta_rs.at[n], dev(dx, dc)).start()

    start_near(0)
    send_meta(idx_all, 0)
    for kb in range(1, AHEAD):
        start_near(kb)
    for kb in range(n_kb):
        across(kb, 0).start()
    for g in range(len(groups)):
        up_load(0, g).start()
    for g in range(len(groups)):
        down_load(0, g).start()

    sub = lax.broadcasted_iota(jnp.int32, (rows_s, n_slot), 0)
    lane = lax.broadcasted_iota(jnp.int32, (rows_s, n_slot), 1)
    my_row = tab[pl.ds(me, 1), :].astype(F32)
    e_col = jnp.sum(jnp.where(sub == lane, my_row, 0.0), axis=1, keepdims=True)
    e_col = jnp.where(sub[:, 0:1] < n_slot, e_col, -2.0)
    total = jnp.zeros((rows_s, n_slot), F32)
    before = jnp.zeros((rows_s, n_slot), F32)
    for d in range(n_dev):
        same = jnp.where(tab[d:d + 1, :].astype(F32) == e_col, 1.0, 0.0)
        total = total + same
        before = before + same * jnp.where(d < me, 1.0, 0.0)
    copies = jnp.sum(total, axis=1, keepdims=True)
    my_rank = jnp.sum(before, axis=1, keepdims=True)
    r = lax.broadcasted_iota(jnp.int32, (cap, LANES), 0)
    for s in range(n_slot):
        want = r.astype(F32) * copies[s:s + 1, :] + my_rank[s:s + 1, :]
        trk[s * cap:(s + 1) * cap, :] = want
    o_odd[...] = jnp.zeros_like(o_odd)

    def clear(q, carry):
        acc[q] = jnp.zeros(acc.shape[1:], F32)
        return carry

    lax.fori_loop(0, acc.shape[0], clear, 0)
    with jax.named_scope("near0"):
        stage_near(0)
    start_near(AHEAD)
    send_meta(gate_all, 1)
    others = pl.ds(1, n_dev - 1)
    with jax.named_scope("meta"):
        arrived(idx_all.at[others], meta_rs.at[0])
    earlier = (lax.broadcasted_iota(jnp.int32, (n_tok, n_tok), 0)
               < lax.broadcasted_iota(jnp.int32, (n_tok, n_tok), 1)).astype(F32).astype(BF16)
    rows_pad = round_up(rows_src, LANES)

    def hits(rank):
        for s in range(n_slot):
            yield s * cap, cap, rank[s:s + 1, :] == trk[s * cap:(s + 1) * cap, 0:1]
        for n in range(odd):
            yield rows_main + n * rows_s, rows_s, rank == float(cap + n) * copies + my_rank

    def route(j, carry):
        idx = idx_all[j].astype(F32)
        has = jnp.zeros((rows_s, n_tok), F32)
        for q in range(n_top):
            has = jnp.where(idx[q:q + 1, :] == e_col, 1.0, has)
        rank = jnp.where(has > 0.0, dot(has.astype(BF16), earlier), -1.0)
        rank_all[j] = rank
        for first, n, hit in hits(rank):
            g_buf[j, first:first + n, :] = jnp.where(hit, 1.0, 0.0).astype(BF16)
        return carry

    def route_gates(j):
        idx = idx_all[j].astype(F32)
        gates = gate_all[j]
        gate = jnp.zeros((rows_s, n_tok), F32)
        for q in range(n_top):
            gate = jnp.where(idx[q:q + 1, :] == e_col, gates[q:q + 1, :], gate)
        parts = []
        for first, n, hit in hits(rank_all[j]):
            s = first // cap
            parts.append(jnp.where(hit, gate[s:s + 1, :] if first < rows_main else gate, 0.0))
        if rows_pad > rows_src:
            parts.append(jnp.zeros((rows_pad - rows_src, n_tok), F32))
        left_over = jnp.transpose(jnp.concatenate(parts, axis=0))[:, :rows_src]
        for n in range(3):
            term = left_over.astype(BF16)
            c_buf[j, n * n_tok:(n + 1) * n_tok, :] = term
            left_over = left_over - term.astype(F32)

    with jax.named_scope("route"):
        lax.fori_loop(0, n_dev, route, 0)
    with jax.named_scope("near1"):
        stage_near(1)
    start_near(AHEAD + 1)
    route_gates(0)
    with jax.named_scope("far0"):
        stage_far(0)
    with jax.named_scope("gates"):
        arrived(gate_all.at[others], meta_rs.at[1])

    chunks = [(n, min(2 * LANES, d_ff - n)) for n in range(0, d_ff, 2 * LANES)]
    n_mid = d_ff // LANES

    def up_block(kb, last, after):
        with jax.named_scope("across"):
            arrived(xall.at[pl.ds(0, CHIPS), kb], sib_rs.at[kb])

        for j in range(n_dev):
            rows = dot(g_buf[j], xall[j, kb])
            main = rows[:rows_main].astype(BF16)
            for s in range(n_slot):
                xg[s, j * cap:(j + 1) * cap, :] = main[s * cap:(s + 1) * cap]
            for n in range(odd):
                first = rows_main + n * rows_s
                for h in range(kb_w // LANES):
                    xg_odd[n, h, pl.ds(j, rows_s, stride=n_dev), :] = rows[first:first + rows_s, h * LANES:(h + 1) * LANES]
        for n in range(odd):
            for h in range(kb_w // LANES):
                for s in range(n_slot):
                    xg[s, d_main + n * n_dev:d_main + (n + 1) * n_dev, h * LANES:(h + 1) * LANES] = (
                        xg_odd[n, h, s * n_dev:(s + 1) * n_dev, :].astype(BF16))
        for g, (s0, n_s) in enumerate(groups):
            with jax.named_scope(f"upload{g}"):
                up_load(kb, g).wait()
            for s in range(s0, s0 + n_s):
                for n0, nw in chunks:
                    v = dot(xg[s], wu[s, :, n0:n0 + nw])
                    for n in range(0, nw, LANES):
                        q = s * n_mid + (n0 + n) // LANES
                        part = acc[q, :d_mid, :] + v[:, n:n + LANES]
                        if last:
                            h_buf[s, :, n0 + n:n0 + n + LANES] = gelu(part).astype(BF16)
                        else:
                            acc[q, :d_mid, :] = part
            if not last:
                up_load(kb + 1, g).start()
            with jax.named_scope(f"stage{g}"):
                if g in after:
                    after[g]()

    def up_step(kb, carry):
        def near_2():
            @pl.when(kb + 2 < n_kb)
            def _():
                stage_near(kb + 2)

            @pl.when(kb + 2 + AHEAD < n_kb)
            def _():
                start_near(kb + 2 + AHEAD)

        def gates():
            for n in range(g_step):
                route_gates(jnp.minimum(kb * g_step + n + 1, n_dev - 1))

        up_block(kb, False, {0: near_2, 1: lambda: stage_far(kb + 1), 2: gates})
        return carry

    g_step = -(-(n_dev - 1) // (n_kb - 1))
    lax.fori_loop(0, n_kb - 1, up_step, 0)
    up_block(n_kb - 1, True, {})

    def mine(cb, off, h):
        return (cb * CHIPS + off) * 2 + h

    def staged(cb, off, h):
        return n_cb * CHIPS * 2 + ((cb % STAGES) * CHIPS + off) * 2 + h

    tok = pl.ds(0, n_tok)

    lots = {2: 0, 1: 1, prev: 1, 0: 2}

    def to_sib(cb, off):
        return rcopy(acc.at[pl.ds(staged(cb, off, 0), 2), tok], sib_in.at[cb, off], ps_ss.at[cb % STAGES], ps_rs.at[cb % 2, lots[off]], sib)

    def to_far(cb):
        return (rcopy(acc.at[mine(cb, 2, 0), tok], far_in.at[cb, 0], out_ss.at[3], pf_rs.at[cb], right),
                rcopy(acc.at[mine(cb, 2, 1), tok], far_in.at[cb, 1], out_ss.at[3], pf_rs.at[cb], left))

    def to_dir(cb):
        return (rcopy(acc.at[mine(cb, 1, 1), tok], sum_in.at[cb, 2], out_ss.at[4], fin_rs.at[cb], right),
                rcopy(acc.at[mine(cb, prev, 0), tok], sum_in.at[cb, 3], out_ss.at[4], fin_rs.at[cb], left))

    def to_mrg(cb):
        return (rcopy(far_in.at[cb, 0], sum_in.at[cb, 0], out_ss.at[5], fin_rs.at[cb], right),
                rcopy(far_in.at[cb, 1], sum_in.at[cb, 1], out_ss.at[5], fin_rs.at[cb], left))

    def merge(cb):
        arrived(far_in.at[cb], pf_rs.at[cb])
        for h, off in ((0, 1), (1, prev)):
            far_in[cb, h] = far_in[cb, h] + acc[mine(cb, off, h), :n_tok, :]
            to_mrg(cb)[h].start()

    def y_copy(cb):
        columns = pl.ds(pl.multiple_of(cb * cb_w, cb_w), cb_w)
        return pltpu.make_async_copy(y_buf.at[cb], y_ref.at[:, columns], y_s.at[cb])

    def finish(cb):
        arrived(sum_in.at[cb], fin_rs.at[cb])
        for h in range(2):
            out = acc[mine(cb, 0, h), :n_tok, :] + sum_in[cb, h] + sum_in[cb, 3 - h]
            y_buf[cb, :, h * LANES:(h + 1) * LANES] = out.astype(BF16)
        y_copy(cb).start()

    def add_sib(cb, off):
        for h in range(2):
            q = mine(cb, off, h)
            acc[q, :n_tok, :] = acc[q, :n_tok, :] + sib_in[cb, off, h]

    def combine(j, q):
        v = dot(c_buf[j], o_buf[j])
        v = (v[2 * n_tok:] + v[n_tok:2 * n_tok]) + v[:n_tok]
        for h in range(2):
            acc[q + h, :n_tok, :] = v[:, h * LANES:(h + 1) * LANES]

    def down_step(cb, carry):
        for g in range(len(groups)):
            down_load(cb, g).wait()
        for g, (s0, n_s) in enumerate(groups):
            for s in range(s0, s0 + n_s):
                out = dot(h_buf[s], wd[s])
                main = out[:d_main].astype(BF16)
                for j in range(n_dev):
                    o_buf[j, s * cap:(s + 1) * cap, :] = main[j * cap:(j + 1) * cap]
                for n in range(odd):
                    first = d_main + n * n_dev
                    for h in range(cb_w // LANES):
                        o_odd[n, h, pl.ds(s, n_dev, stride=rows_s), :] = out[first:first + n_dev, h * LANES:(h + 1) * LANES]


        for n in range(odd):
            first = rows_main + n * rows_s
            for h in range(cb_w // LANES):
                for j in range(n_dev):
                    o_buf[j, first:first + rows_s, h * LANES:(h + 1) * LANES] = o_odd[n, h, j * rows_s:(j + 1) * rows_s, :].astype(BF16)

        @pl.when(cb >= STAGES)
        def _():
            took(acc.at[pl.ds(staged(cb, 0, 0), 2 * CHIPS), tok], ps_ss.at[cb % STAGES])

        @pl.when(cb + 1 < n_cb)
        def _():
            for g in range(len(groups)):
                down_load(cb + 1, g).start()

        with jax.named_scope("merge0"):
            @pl.when(cb == 1)
            def _():
                merge(cb - 1)

        def for_sib(off):
            combine(2 * off + 1, staged(cb, off, 0))
            to_sib(cb, off).start()

        for off in (2, 1, prev):
            for_sib(off)
        combine(2 * 2, mine(cb, 2, 0))
        with jax.named_scope("sibF"):
            arrived(sib_in.at[cb, 2], ps_rs.at[cb % 2, 0])
        add_sib(cb, 2)
        for c in to_far(cb):
            c.start()
        for_sib(0)
        for off in (1, prev):
            combine(2 * off, mine(cb, off, 0))
        with jax.named_scope("sibRL"):
            arrived(sib_in.at[cb, pl.ds(0, 2)], ps_rs.at[cb % 2, 1])
        for n, off in enumerate((1, prev)):
            add_sib(cb, off)
            to_dir(cb)[n].start()
        combine(0, mine(cb, 0, 0))

        @pl.when(cb >= LAG)
        def _():
            finish(cb - LAG)

        arrived(sib_in.at[cb, 0], ps_rs.at[cb % 2, 2])
        add_sib(cb, 0)

        with jax.named_scope("merge"):
            @pl.when(cb >= 2)
            def _():
                merge(cb - 1)
        return carry

    lax.fori_loop(0, n_cb, down_step, 0)
    with jax.named_scope("merge_last"):
        merge(n_cb - 1)
    with jax.named_scope("finish_last"):
        for cb in range(max(0, n_cb - LAG), n_cb):
            finish(cb)

    took(idx_all.at[others], meta_ss.at[0])
    took(gate_all.at[others], meta_ss.at[1])
    for n, ref in enumerate((xall.at[pl.ds(0, 2)], xall.at[4], xall.at[pl.ds(0, CHIPS)], far_in, far_in, far_in)):
        took(ref, out_ss.at[n])
    for n in range(min(STAGES, n_cb)):
        took(acc.at[pl.ds(staged(n, 0, 0), 2 * CHIPS), tok], ps_ss.at[n])
    for cb in range(n_cb):
        y_copy(cb).wait()


def solution(mesh):
    assert mesh.shape["ep"] == 2 * CHIPS

    def group_layer(tokens, topk_idx, topk_w, w_up, w_down, slot_expert):
        n_tok, d_model = tokens.shape
        n_top = topk_idx.shape[1]
        n_dev, n_slot = slot_expert.shape
        d_ff = w_up.shape[-1]
        bound = slot_bound(n_tok, n_top, n_dev, n_slot)
        cap = bound // 8 * 8
        odd, rows_s = bound - cap, round_up(n_slot, 16)
        kb_w, cb_w = 2 * LANES, 2 * LANES
        n_kb, n_cb = d_model // kb_w, d_model // cb_w
        d_mid = n_dev * bound
        rows_src = n_slot * cap + odd * rows_s
        n_acc = max(n_slot * (d_ff // LANES), (n_cb + STAGES) * CHIPS * 2)
        cfg = dict(bound=bound, cap=cap, kb_w=kb_w, cb_w=cb_w)
        dma = pltpu.SemaphoreType.DMA
        hbm = pl.BlockSpec(memory_space=pl.ANY)
        return pl.pallas_call(
            functools.partial(moe_kernel, cfg),
            out_shape=jax.ShapeDtypeStruct((n_tok, d_model), BF16),
            in_specs=[hbm] * 6,
            out_specs=hbm,
            scratch_shapes=[
                pltpu.VMEM((n_dev, n_kb, n_tok, kb_w), BF16),
                pltpu.VMEM((n_dev, n_top, n_tok), jnp.int32),
                pltpu.VMEM((n_dev, n_top, n_tok), F32),
                pltpu.VMEM((n_dev, rows_s, n_tok), F32),
                pltpu.VMEM((n_dev, n_slot), jnp.int32),
                pltpu.VMEM((n_slot * cap, LANES), F32),
                pltpu.VMEM((n_dev, rows_src, n_tok), BF16),
                pltpu.VMEM((n_dev, 3 * n_tok, rows_src), BF16),
                pltpu.VMEM((n_slot, d_mid, kb_w), BF16),
                pltpu.VMEM((odd, kb_w // LANES, rows_s * n_dev, LANES), F32),
                pltpu.VMEM((n_acc, max(d_mid, n_tok), LANES), F32),
                pltpu.VMEM((n_slot, d_mid, d_ff), BF16),
                pltpu.VMEM((n_dev, rows_src, cb_w), BF16),
                pltpu.VMEM((odd, cb_w // LANES, n_dev * rows_s, LANES), F32),
                pltpu.VMEM((n_slot, kb_w, d_ff), BF16),
                pltpu.VMEM((n_slot, d_ff, cb_w), BF16),
                pltpu.VMEM((n_cb, CHIPS, 2, n_tok, LANES), F32),
                pltpu.VMEM((n_cb, 2, n_tok, LANES), F32),
                pltpu.VMEM((n_cb, 4, n_tok, LANES), F32),
                pltpu.VMEM((n_cb, n_tok, cb_w), BF16),
                dma((4,)), dma((2,)), dma((2,)), dma((6,)),
                dma((n_kb,)), dma((n_kb,)), dma((n_kb,)),
                dma((-(-n_slot // GROUP),)), dma((-(-n_slot // GROUP),)),
                dma((STAGES,)), dma((2, 3)), dma((n_cb,)), dma((n_cb,)), dma((n_cb,)),
            ],
            compiler_params=pltpu.CompilerParams(collective_id=0, has_side_effects=True, vmem_limit_bytes=67_000_000),
        )(tokens, topk_idx.T, topk_w.T, slot_expert, w_up, w_down)

    row_spec = P(('dp', 'ep'), None)
    weight_spec = P('ep', None, None, None)
    return jax.shard_map(group_layer, mesh=mesh, in_specs=(row_spec, row_spec, row_spec, weight_spec, weight_spec, P(None, None)),
                         out_specs=row_spec, check_vma=False)
```

```python
import functools

import jax
import jax.numpy as jnp
from jax import lax
from jax.experimental import pallas as pl
from jax.experimental.pallas import tpu as pltpu
from jax.sharding import PartitionSpec as P

MESH = pl.DeviceIdType.MESH
F32 = jnp.float32
BF16 = jnp.bfloat16
LANES = 128
CHIPS = 4
AHEAD = 2
STAGES = 4
GROUP = 3
LAG = 3


def slot_bound(n_tok, n_top, n_dev, n_slot):
    base_load = (n_tok * n_top) // (n_dev * n_slot)
    return base_load + base_load // 2 + 1


def round_up(n, m):
    return -(-n // m) * m


def gelu(v):
    return v * (0.5 + 0.5 * jnp.tanh(v * (0.7978845608028654 + (0.7978845608028654 * 0.044715) * (v * v))))


def dot(a, b):
    return lax.dot_general(a, b, (((1,), (0,)), ((), ())), preferred_element_type=F32)


def moe_kernel(cfg, x_ref, idx_ref, gate_ref, tab_ref, wup_ref, wdn_ref, y_ref,
               xall, idx_all, gate_all, rank_all, tab, trk, g_buf, c_buf, xg, xg_odd, acc, h_buf, o_buf, o_odd, wu, wd, sib_in, far_in, sum_in, y_buf,
               in_s, meta_ss, meta_rs, out_ss, near_rs, rel_rs, sib_rs, wu_s, wd_s, ps_ss, ps_rs, pf_rs, fin_rs, y_s):
    bound, cap, kb_w, cb_w = (cfg[k] for k in ("bound", "cap", "kb_w", "cb_w"))
    odd = bound - cap
    n_tok, d_model = x_ref.shape
    n_top = idx_ref.shape[0]
    n_dev, n_slot = tab_ref.shape
    d_ff = wup_ref.shape[-1]
    d_main, d_mid = n_dev * cap, n_dev * bound
    rows_s = round_up(n_slot, 16)
    rows_main, rows_src = n_slot * cap, n_slot * cap + odd * rows_s
    n_kb, n_cb = d_model // kb_w, d_model // cb_w
    half = n_tok // 2
    me = lax.axis_index("ep")
    chip, core = me // 2, me % 2

    def dev(d_chip, d_core=0):
        return {"ep": ((chip + d_chip) % CHIPS) * 2 + (core + d_core) % 2}

    right, left, sib = dev(1), dev(CHIPS - 1), dev(0, 1)

    def rcopy(src, dst, ss, rs, to):
        return pltpu.make_async_remote_copy(src_ref=src, dst_ref=dst, send_sem=ss, recv_sem=rs, device_id=to, device_id_type=MESH)

    def took(ref, sem):
        rcopy(ref, ref, sem, sem, sib).wait_send()

    def arrived(ref, sem):
        rcopy(ref, ref, sem, sem, sib).wait_recv()

    groups = [(s, min(GROUP, n_slot - s)) for s in range(0, n_slot, GROUP)]

    class Loads:
        def __init__(self, src, dst, sem, g):
            (s, n), self.src, self.dst, self.sem = groups[g], src, dst, sem.at[g]
            self.slots, self.all = range(s, s + n), pl.ds(s, n)

        def start(self):
            for s in self.slots:
                pltpu.make_async_copy(self.src(s), self.dst.at[s], self.sem).start()

        def wait(self):
            pltpu.make_async_copy(self.src(self.all), self.dst.at[self.all], self.sem).wait()

    def up_load(kb, g):
        return Loads(lambda s: wup_ref.at[0, s, pl.ds(pl.multiple_of(kb * kb_w, kb_w), kb_w), :], wu, wu_s, g)

    def down_load(cb, g):
        return Loads(lambda s: wdn_ref.at[0, s, :, pl.ds(pl.multiple_of(cb * cb_w, cb_w), cb_w)], wd, wd_s, g)

    barrier = pltpu.get_barrier_semaphore()
    peers = [(1, 0), (2, 0), (CHIPS - 1, 0), (0, 1)]
    for dx, dc in peers:
        pl.semaphore_signal(barrier, inc=1, device_id=dev(dx, dc), device_id_type=MESH)
    in_meta = [pltpu.make_async_copy(idx_ref, idx_all.at[0], in_s.at[1]), pltpu.make_async_copy(gate_ref, gate_all.at[0], in_s.at[2]),
               pltpu.make_async_copy(tab_ref, tab, in_s.at[3])]
    for c in in_meta:
        c.start()
    for kb in range(n_kb):
        pltpu.make_async_copy(x_ref.at[:, pl.ds(kb * kb_w, kb_w)], xall.at[0, kb], in_s.at[0]).start()
    arrived(xall.at[0], in_s.at[0])
    for c in in_meta:
        c.wait()
    pl.semaphore_wait(barrier, len(peers))

    lo, hi = pl.ds(0, half), pl.ds(half, n_tok - half)
    prev = CHIPS - 1

    def near(kb):
        return (rcopy(xall.at[0, kb], xall.at[2 * prev, kb], out_ss.at[0], near_rs.at[kb], right),
                rcopy(xall.at[0, kb], xall.at[2, kb], out_ss.at[0], near_rs.at[kb], left))

    def relay(kb):
        return (rcopy(xall.at[2 * prev, kb, lo], xall.at[4, kb, lo], out_ss.at[1], rel_rs.at[kb], right),
                rcopy(xall.at[2, kb, hi], xall.at[4, kb, hi], out_ss.at[1], rel_rs.at[kb], left))

    def across(kb, off):
        return rcopy(xall.at[2 * off, kb], xall.at[2 * off + 1, kb], out_ss.at[2], sib_rs.at[kb], sib)

    def start_near(kb):
        for c in near(kb):
            c.start()

    def stage_near(kb):
        arrived(xall.at[pl.ds(0, 2), kb], near_rs.at[kb])
        for c in relay(kb):
            c.start()
        for off in (prev, 1):
            across(kb, off).start()

    def stage_far(kb):
        arrived(xall.at[4, kb], rel_rs.at[kb])
        across(kb, 2).start()

    def send_meta(ref, n):
        for dx in range(1, CHIPS):
            rcopy(ref.at[0], ref.at[2 * (CHIPS - dx)], meta_ss.at[n], meta_rs.at[n, 0], dev(dx)).start()
        rcopy(ref.at[0], ref.at[1], meta_ss.at[n], meta_rs.at[n, 1], sib).start()

    def hand_meta(ref, n):
        arrived(ref.at[pl.ds(0, CHIPS - 1)], meta_rs.at[n, 0])
        for off in range(1, CHIPS):
            rcopy(ref.at[2 * off], ref.at[2 * off + 1], meta_ss.at[n], meta_rs.at[n, 1], sib).start()

    def wait_meta(ref, n):
        arrived(ref.at[pl.ds(0, CHIPS)], meta_rs.at[n, 1])

    start_near(0)
    send_meta(idx_all, 0)
    for kb in range(1, AHEAD):
        start_near(kb)
    for kb in range(n_kb):
        across(kb, 0).start()
    for g in range(len(groups)):
        up_load(0, g).start()
    for g in range(len(groups)):
        down_load(0, g).start()

    sub = lax.broadcasted_iota(jnp.int32, (rows_s, n_slot), 0)
    lane = lax.broadcasted_iota(jnp.int32, (rows_s, n_slot), 1)
    my_row = tab[pl.ds(me, 1), :].astype(F32)
    e_col = jnp.sum(jnp.where(sub == lane, my_row, 0.0), axis=1, keepdims=True)
    e_col = jnp.where(sub[:, 0:1] < n_slot, e_col, -2.0)
    total = jnp.zeros((rows_s, n_slot), F32)
    before = jnp.zeros((rows_s, n_slot), F32)
    for d in range(n_dev):
        same = jnp.where(tab[d:d + 1, :].astype(F32) == e_col, 1.0, 0.0)
        total = total + same
        before = before + same * jnp.where(d < me, 1.0, 0.0)
    copies = jnp.sum(total, axis=1, keepdims=True)
    my_rank = jnp.sum(before, axis=1, keepdims=True)
    r = lax.broadcasted_iota(jnp.int32, (cap, LANES), 0)
    for s in range(n_slot):
        want = r.astype(F32) * copies[s:s + 1, :] + my_rank[s:s + 1, :]
        trk[s * cap:(s + 1) * cap, :] = want
    o_odd[...] = jnp.zeros_like(o_odd)

    def clear(q, carry):
        acc[q] = jnp.zeros(acc.shape[1:], F32)
        return carry

    lax.fori_loop(0, acc.shape[0], clear, 0)
    stage_near(0)
    start_near(AHEAD)
    hand_meta(idx_all, 0)
    wait_meta(idx_all, 0)
    earlier = (lax.broadcasted_iota(jnp.int32, (n_tok, n_tok), 0)
               < lax.broadcasted_iota(jnp.int32, (n_tok, n_tok), 1)).astype(F32).astype(BF16)
    rows_pad = round_up(rows_src, LANES)

    def hits(rank):
        for s in range(n_slot):
            yield s * cap, cap, rank[s:s + 1, :] == trk[s * cap:(s + 1) * cap, 0:1]
        for n in range(odd):
            yield rows_main + n * rows_s, rows_s, rank == float(cap + n) * copies + my_rank

    def route(j, carry):
        idx = idx_all[j].astype(F32)
        has = jnp.zeros((rows_s, n_tok), F32)
        for q in range(n_top):
            has = jnp.where(idx[q:q + 1, :] == e_col, 1.0, has)
        rank = jnp.where(has > 0.0, dot(has.astype(BF16), earlier), -1.0)
        rank_all[j] = rank
        for first, n, hit in hits(rank):
            g_buf[j, first:first + n, :] = jnp.where(hit, 1.0, 0.0).astype(BF16)
        return carry

    def route_gates(j):
        idx = idx_all[j].astype(F32)
        gates = gate_all[j]
        gate = jnp.zeros((rows_s, n_tok), F32)
        for q in range(n_top):
            gate = jnp.where(idx[q:q + 1, :] == e_col, gates[q:q + 1, :], gate)
        parts = []
        for first, n, hit in hits(rank_all[j]):
            s = first // cap
            parts.append(jnp.where(hit, gate[s:s + 1, :] if first < rows_main else gate, 0.0))
        if rows_pad > rows_src:
            parts.append(jnp.zeros((rows_pad - rows_src, n_tok), F32))
        left_over = jnp.transpose(jnp.concatenate(parts, axis=0))[:, :rows_src]
        for n in range(3):
            term = left_over.astype(BF16)
            c_buf[j, n * n_tok:(n + 1) * n_tok, :] = term
            left_over = left_over - term.astype(F32)

    lax.fori_loop(0, n_dev, route, 0)
    stage_near(1)
    start_near(AHEAD + 1)
    send_meta(gate_all, 1)
    route_gates(0)
    stage_far(0)

    chunks = [(n, min(2 * LANES, d_ff - n)) for n in range(0, d_ff, 2 * LANES)]
    n_mid = d_ff // LANES

    def up_block(kb, last, after):
        arrived(xall.at[pl.ds(0, CHIPS), kb], sib_rs.at[kb])

        for j in range(n_dev):
            rows = dot(g_buf[j], xall[j, kb])
            main = rows[:rows_main].astype(BF16)
            for s in range(n_slot):
                xg[s, j * cap:(j + 1) * cap, :] = main[s * cap:(s + 1) * cap]
            for n in range(odd):
                first = rows_main + n * rows_s
                for h in range(kb_w // LANES):
                    xg_odd[n, h, pl.ds(j, rows_s, stride=n_dev), :] = rows[first:first + rows_s, h * LANES:(h + 1) * LANES]
        for n in range(odd):
            for h in range(kb_w // LANES):
                for s in range(n_slot):
                    xg[s, d_main + n * n_dev:d_main + (n + 1) * n_dev, h * LANES:(h + 1) * LANES] = (
                        xg_odd[n, h, s * n_dev:(s + 1) * n_dev, :].astype(BF16))
        for g, (s0, n_s) in enumerate(groups):
            up_load(kb, g).wait()
            for s in range(s0, s0 + n_s):
                for n0, nw in chunks:
                    v = dot(xg[s], wu[s, :, n0:n0 + nw])
                    for n in range(0, nw, LANES):
                        q = s * n_mid + (n0 + n) // LANES
                        part = acc[q, :d_mid, :] + v[:, n:n + LANES]
                        if last:
                            h_buf[s, :, n0 + n:n0 + n + LANES] = gelu(part).astype(BF16)
                        else:
                            acc[q, :d_mid, :] = part
            if not last:
                up_load(kb + 1, g).start()
            if g in after:
                after[g]()

    def up_step(kb, carry):
        def near_2():
            @pl.when(kb + 2 < n_kb)
            def _():
                stage_near(kb + 2)

            @pl.when(kb + 2 + AHEAD < n_kb)
            def _():
                start_near(kb + 2 + AHEAD)

        def gates():
            @pl.when(kb == 1)
            def _():
                hand_meta(gate_all, 1)

            @pl.when(kb == 2)
            def _():
                wait_meta(gate_all, 1)

            @pl.when((kb >= 2) & (kb < 2 + n_dev // 2))
            def _():
                route_gates(2 * (kb - 2) + 1)
                route_gates(jnp.minimum(2 * (kb - 2) + 2, n_dev - 1))

        up_block(kb, False, {0: near_2, 1: lambda: stage_far(kb + 1), 2: gates})
        return carry

    assert n_kb - 1 >= 2 + n_dev // 2
    lax.fori_loop(0, n_kb - 1, up_step, 0)
    up_block(n_kb - 1, True, {})

    def mine(cb, off, h):
        return (cb * CHIPS + off) * 2 + h

    def staged(cb, off, h):
        return n_cb * CHIPS * 2 + ((cb % STAGES) * CHIPS + off) * 2 + h

    tok = pl.ds(0, n_tok)

    lots = {2: 0, 1: 1, prev: 1, 0: 2}

    def to_sib(cb, off):
        return rcopy(acc.at[pl.ds(staged(cb, off, 0), 2), tok], sib_in.at[cb, off], ps_ss.at[cb % STAGES], ps_rs.at[cb % 2, lots[off]], sib)

    def to_far(cb):
        return (rcopy(acc.at[mine(cb, 2, 0), tok], far_in.at[cb, 0], out_ss.at[3], pf_rs.at[cb], right),
                rcopy(acc.at[mine(cb, 2, 1), tok], far_in.at[cb, 1], out_ss.at[3], pf_rs.at[cb], left))

    def to_dir(cb):
        return (rcopy(acc.at[mine(cb, 1, 1), tok], sum_in.at[cb, 2], out_ss.at[4], fin_rs.at[cb], right),
                rcopy(acc.at[mine(cb, prev, 0), tok], sum_in.at[cb, 3], out_ss.at[4], fin_rs.at[cb], left))

    def to_mrg(cb):
        return (rcopy(far_in.at[cb, 0], sum_in.at[cb, 0], out_ss.at[5], fin_rs.at[cb], right),
                rcopy(far_in.at[cb, 1], sum_in.at[cb, 1], out_ss.at[5], fin_rs.at[cb], left))

    def merge(cb):
        arrived(far_in.at[cb], pf_rs.at[cb])
        for h, off in ((0, 1), (1, prev)):
            far_in[cb, h] = far_in[cb, h] + acc[mine(cb, off, h), :n_tok, :]
            to_mrg(cb)[h].start()

    def y_copy(cb):
        columns = pl.ds(pl.multiple_of(cb * cb_w, cb_w), cb_w)
        return pltpu.make_async_copy(y_buf.at[cb], y_ref.at[:, columns], y_s.at[cb])

    def finish(cb):
        arrived(sum_in.at[cb], fin_rs.at[cb])
        for h in range(2):
            out = acc[mine(cb, 0, h), :n_tok, :] + sum_in[cb, h] + sum_in[cb, 3 - h]
            y_buf[cb, :, h * LANES:(h + 1) * LANES] = out.astype(BF16)
        y_copy(cb).start()

    def add_sib(cb, off):
        for h in range(2):
            q = mine(cb, off, h)
            acc[q, :n_tok, :] = acc[q, :n_tok, :] + sib_in[cb, off, h]

    def combine(j, q):
        v = dot(c_buf[j], o_buf[j])
        v = (v[2 * n_tok:] + v[n_tok:2 * n_tok]) + v[:n_tok]
        for h in range(2):
            acc[q + h, :n_tok, :] = v[:, h * LANES:(h + 1) * LANES]

    def down_step(cb, carry):
        for g in range(len(groups)):
            down_load(cb, g).wait()
        for g, (s0, n_s) in enumerate(groups):
            for s in range(s0, s0 + n_s):
                out = dot(h_buf[s], wd[s])
                main = out[:d_main].astype(BF16)
                for j in range(n_dev):
                    o_buf[j, s * cap:(s + 1) * cap, :] = main[j * cap:(j + 1) * cap]
                for n in range(odd):
                    first = d_main + n * n_dev
                    for h in range(cb_w // LANES):
                        o_odd[n, h, pl.ds(s, n_dev, stride=rows_s), :] = out[first:first + n_dev, h * LANES:(h + 1) * LANES]


        for n in range(odd):
            first = rows_main + n * rows_s
            for h in range(cb_w // LANES):
                for j in range(n_dev):
                    o_buf[j, first:first + rows_s, h * LANES:(h + 1) * LANES] = o_odd[n, h, j * rows_s:(j + 1) * rows_s, :].astype(BF16)

        @pl.when(cb >= STAGES)
        def _():
            took(acc.at[pl.ds(staged(cb, 0, 0), 2 * CHIPS), tok], ps_ss.at[cb % STAGES])

        @pl.when(cb + 1 < n_cb)
        def _():
            for g in range(len(groups)):
                down_load(cb + 1, g).start()

        @pl.when(cb == 1)
        def _():
            merge(cb - 1)

        def for_sib(off):
            combine(2 * off + 1, staged(cb, off, 0))
            to_sib(cb, off).start()

        for off in (2, 1, prev):
            for_sib(off)
        combine(2 * 2, mine(cb, 2, 0))
        arrived(sib_in.at[cb, 2], ps_rs.at[cb % 2, 0])
        add_sib(cb, 2)
        for c in to_far(cb):
            c.start()
        for_sib(0)
        for off in (1, prev):
            combine(2 * off, mine(cb, off, 0))
        arrived(sib_in.at[cb, pl.ds(0, 2)], ps_rs.at[cb % 2, 1])
        for n, off in enumerate((1, prev)):
            add_sib(cb, off)
            to_dir(cb)[n].start()
        combine(0, mine(cb, 0, 0))

        @pl.when(cb >= LAG)
        def _():
            finish(cb - LAG)

        arrived(sib_in.at[cb, 0], ps_rs.at[cb % 2, 2])
        add_sib(cb, 0)

        @pl.when(cb >= 2)
        def _():
            merge(cb - 1)
        return carry

    lax.fori_loop(0, n_cb, down_step, 0)
    merge(n_cb - 1)
    for cb in range(max(0, n_cb - LAG), n_cb):
        finish(cb)

    others = pl.ds(1, n_dev - 1)
    took(idx_all.at[others], meta_ss.at[0])
    took(gate_all.at[others], meta_ss.at[1])
    for n, ref in enumerate((xall.at[pl.ds(0, 2)], xall.at[4], xall.at[pl.ds(0, CHIPS)], far_in, far_in, far_in)):
        took(ref, out_ss.at[n])
    for n in range(min(STAGES, n_cb)):
        took(acc.at[pl.ds(staged(n, 0, 0), 2 * CHIPS), tok], ps_ss.at[n])
    for cb in range(n_cb):
        y_copy(cb).wait()


def solution(mesh):
    assert mesh.shape["ep"] == 2 * CHIPS

    def group_layer(tokens, topk_idx, topk_w, w_up, w_down, slot_expert):
        n_tok, d_model = tokens.shape
        n_top = topk_idx.shape[1]
        n_dev, n_slot = slot_expert.shape
        d_ff = w_up.shape[-1]
        bound = slot_bound(n_tok, n_top, n_dev, n_slot)
        cap = bound // 8 * 8
        odd, rows_s = bound - cap, round_up(n_slot, 16)
        kb_w, cb_w = 2 * LANES, 2 * LANES
        n_kb, n_cb = d_model // kb_w, d_model // cb_w
        d_mid = n_dev * bound
        rows_src = n_slot * cap + odd * rows_s
        n_acc = max(n_slot * (d_ff // LANES), (n_cb + STAGES) * CHIPS * 2)
        cfg = dict(bound=bound, cap=cap, kb_w=kb_w, cb_w=cb_w)
        dma = pltpu.SemaphoreType.DMA
        hbm = pl.BlockSpec(memory_space=pl.ANY)
        return pl.pallas_call(
            functools.partial(moe_kernel, cfg),
            out_shape=jax.ShapeDtypeStruct((n_tok, d_model), BF16),
            in_specs=[hbm] * 6,
            out_specs=hbm,
            scratch_shapes=[
                pltpu.VMEM((n_dev, n_kb, n_tok, kb_w), BF16),
                pltpu.VMEM((n_dev, n_top, n_tok), jnp.int32),
                pltpu.VMEM((n_dev, n_top, n_tok), F32),
                pltpu.VMEM((n_dev, rows_s, n_tok), F32),
                pltpu.VMEM((n_dev, n_slot), jnp.int32),
                pltpu.VMEM((n_slot * cap, LANES), F32),
                pltpu.VMEM((n_dev, rows_src, n_tok), BF16),
                pltpu.VMEM((n_dev, 3 * n_tok, rows_src), BF16),
                pltpu.VMEM((n_slot, d_mid, kb_w), BF16),
                pltpu.VMEM((odd, kb_w // LANES, rows_s * n_dev, LANES), F32),
                pltpu.VMEM((n_acc, max(d_mid, n_tok), LANES), F32),
                pltpu.VMEM((n_slot, d_mid, d_ff), BF16),
                pltpu.VMEM((n_dev, rows_src, cb_w), BF16),
                pltpu.VMEM((odd, cb_w // LANES, n_dev * rows_s, LANES), F32),
                pltpu.VMEM((n_slot, kb_w, d_ff), BF16),
                pltpu.VMEM((n_slot, d_ff, cb_w), BF16),
                pltpu.VMEM((n_cb, CHIPS, 2, n_tok, LANES), F32),
                pltpu.VMEM((n_cb, 2, n_tok, LANES), F32),
                pltpu.VMEM((n_cb, 4, n_tok, LANES), F32),
                pltpu.VMEM((n_cb, n_tok, cb_w), BF16),
                dma((4,)), dma((2,)), dma((2, 2)), dma((6,)),
                dma((n_kb,)), dma((n_kb,)), dma((n_kb,)),
                dma((-(-n_slot // GROUP),)), dma((-(-n_slot // GROUP),)),
                dma((STAGES,)), dma((2, 3)), dma((n_cb,)), dma((n_cb,)), dma((n_cb,)),
            ],
            compiler_params=pltpu.CompilerParams(collective_id=0, has_side_effects=True, vmem_limit_bytes=67_000_000),
        )(tokens, topk_idx.T, topk_w.T, slot_expert, w_up, w_down)

    row_spec = P(('dp', 'ep'), None)
    weight_spec = P('ep', None, None, None)
    return jax.shard_map(group_layer, mesh=mesh, in_specs=(row_spec, row_spec, row_spec, weight_spec, weight_spec, P(None, None)),
                         out_specs=row_spec, check_vma=False)
```

```python
import functools

import jax
import jax.numpy as jnp
from jax import lax
from jax.experimental import pallas as pl
from jax.experimental.pallas import tpu as pltpu
from jax.sharding import PartitionSpec as P

MESH = pl.DeviceIdType.MESH
F32 = jnp.float32
BF16 = jnp.bfloat16
LANES = 128
CHIPS = 4
AHEAD = 2
STAGES = 4
GROUP = 3
LAG = 3


def slot_bound(n_tok, n_top, n_dev, n_slot):
    base_load = (n_tok * n_top) // (n_dev * n_slot)
    return base_load + base_load // 2 + 1


def round_up(n, m):
    return -(-n // m) * m


def gelu(v):
    return v * (0.5 + 0.5 * jnp.tanh(v * (0.7978845608028654 + (0.7978845608028654 * 0.044715) * (v * v))))


def dot(a, b):
    return lax.dot_general(a, b, (((1,), (0,)), ((), ())), preferred_element_type=F32)


def moe_kernel(cfg, x_ref, idx_ref, gate_ref, tab_ref, wup_ref, wdn_ref, y_ref,
               xall, idx_all, gate_all, rank_all, tab, trk, g_buf, c_buf, xg, xg_odd, acc, h_buf, o_buf, o_odd, wu, wd, sib_in, far_in, sum_in, y_buf,
               in_s, meta_ss, meta_rs, out_ss, near_rs, rel_rs, sib_rs, wu_s, wd_s, ps_ss, ps_rs, pf_rs, fin_rs, y_s):
    bound, cap, kb_w, cb_w = (cfg[k] for k in ("bound", "cap", "kb_w", "cb_w"))
    odd = bound - cap
    n_tok, d_model = x_ref.shape
    n_top = idx_ref.shape[0]
    n_dev, n_slot = tab_ref.shape
    d_ff = wup_ref.shape[-1]
    d_main, d_mid = n_dev * cap, n_dev * bound
    rows_s = round_up(n_slot, 16)
    rows_main, rows_src = n_slot * cap, n_slot * cap + odd * rows_s
    n_kb, n_cb = d_model // kb_w, d_model // cb_w
    half = n_tok // 2
    me = lax.axis_index("ep")
    chip, core = me // 2, me % 2

    def dev(d_chip, d_core=0):
        return {"ep": ((chip + d_chip) % CHIPS) * 2 + (core + d_core) % 2}

    right, left, sib = dev(1), dev(CHIPS - 1), dev(0, 1)

    def rcopy(src, dst, ss, rs, to):
        return pltpu.make_async_remote_copy(src_ref=src, dst_ref=dst, send_sem=ss, recv_sem=rs, device_id=to, device_id_type=MESH)

    def took(ref, sem):
        rcopy(ref, ref, sem, sem, sib).wait_send()

    def arrived(ref, sem):
        rcopy(ref, ref, sem, sem, sib).wait_recv()

    groups = [(s, min(GROUP, n_slot - s)) for s in range(0, n_slot, GROUP)]

    class Loads:
        def __init__(self, src, dst, sem, g):
            (s, n), self.src, self.dst, self.sem = groups[g], src, dst, sem.at[g]
            self.slots, self.all = range(s, s + n), pl.ds(s, n)

        def start(self):
            for s in self.slots:
                pltpu.make_async_copy(self.src(s), self.dst.at[s], self.sem).start()

        def wait(self):
            pltpu.make_async_copy(self.src(self.all), self.dst.at[self.all], self.sem).wait()

    def up_load(kb, g):
        return Loads(lambda s: wup_ref.at[0, s, pl.ds(pl.multiple_of(kb * kb_w, kb_w), kb_w), :], wu, wu_s, g)

    def down_load(cb, g):
        return Loads(lambda s: wdn_ref.at[0, s, :, pl.ds(pl.multiple_of(cb * cb_w, cb_w), cb_w)], wd, wd_s, g)

    barrier = pltpu.get_barrier_semaphore()
    peers = [(1, 0), (2, 0), (CHIPS - 1, 0), (0, 1)]
    for dx, dc in peers:
        pl.semaphore_signal(barrier, inc=1, device_id=dev(dx, dc), device_id_type=MESH)
    in_meta = [pltpu.make_async_copy(idx_ref, idx_all.at[0], in_s.at[1]), pltpu.make_async_copy(gate_ref, gate_all.at[0], in_s.at[2]),
               pltpu.make_async_copy(tab_ref, tab, in_s.at[3])]
    for c in in_meta:
        c.start()
    for kb in range(n_kb):
        pltpu.make_async_copy(x_ref.at[:, pl.ds(kb * kb_w, kb_w)], xall.at[0, kb], in_s.at[0]).start()
    arrived(xall.at[0], in_s.at[0])
    for c in in_meta:
        c.wait()
    pl.semaphore_wait(barrier, len(peers))

    lo, hi = pl.ds(0, half), pl.ds(half, n_tok - half)
    prev = CHIPS - 1

    def near(kb):
        return (rcopy(xall.at[0, kb], xall.at[2 * prev, kb], out_ss.at[0], near_rs.at[kb], right),
                rcopy(xall.at[0, kb], xall.at[2, kb], out_ss.at[0], near_rs.at[kb], left))

    def relay(kb):
        return (rcopy(xall.at[2 * prev, kb, lo], xall.at[4, kb, lo], out_ss.at[1], rel_rs.at[kb], right),
                rcopy(xall.at[2, kb, hi], xall.at[4, kb, hi], out_ss.at[1], rel_rs.at[kb], left))

    def across(kb, off):
        return rcopy(xall.at[2 * off, kb], xall.at[2 * off + 1, kb], out_ss.at[2], sib_rs.at[kb], sib)

    def start_near(kb):
        for c in near(kb):
            c.start()

    def stage_near(kb):
        arrived(xall.at[pl.ds(0, 2), kb], near_rs.at[kb])
        for c in relay(kb):
            c.start()
        for off in (prev, 1):
            across(kb, off).start()

    def stage_far(kb):
        arrived(xall.at[4, kb], rel_rs.at[kb])
        across(kb, 2).start()

    def send_meta(ref, n):
        for dx in range(1, CHIPS):
            rcopy(ref.at[0], ref.at[2 * (CHIPS - dx)], meta_ss.at[n], meta_rs.at[n, 0], dev(dx)).start()
        rcopy(ref.at[0], ref.at[1], meta_ss.at[n], meta_rs.at[n, 1], sib).start()

    def hand_meta(ref, n):
        arrived(ref.at[pl.ds(0, CHIPS - 1)], meta_rs.at[n, 0])
        for off in range(1, CHIPS):
            rcopy(ref.at[2 * off], ref.at[2 * off + 1], meta_ss.at[n], meta_rs.at[n, 1], sib).start()

    def wait_meta(ref, n):
        arrived(ref.at[pl.ds(0, CHIPS)], meta_rs.at[n, 1])

    start_near(0)
    send_meta(idx_all, 0)
    for kb in range(1, AHEAD):
        start_near(kb)
    for kb in range(n_kb):
        across(kb, 0).start()
    for g in range(len(groups)):
        up_load(0, g).start()
    for g in range(len(groups)):
        down_load(0, g).start()

    sub = lax.broadcasted_iota(jnp.int32, (rows_s, n_slot), 0)
    lane = lax.broadcasted_iota(jnp.int32, (rows_s, n_slot), 1)
    my_row = tab[pl.ds(me, 1), :].astype(F32)
    e_col = jnp.sum(jnp.where(sub == lane, my_row, 0.0), axis=1, keepdims=True)
    e_col = jnp.where(sub[:, 0:1] < n_slot, e_col, -2.0)
    total = jnp.zeros((rows_s, n_slot), F32)
    before = jnp.zeros((rows_s, n_slot), F32)
    for d in range(n_dev):
        same = jnp.where(tab[d:d + 1, :].astype(F32) == e_col, 1.0, 0.0)
        total = total + same
        before = before + same * jnp.where(d < me, 1.0, 0.0)
    copies = jnp.sum(total, axis=1, keepdims=True)
    my_rank = jnp.sum(before, axis=1, keepdims=True)
    r = lax.broadcasted_iota(jnp.int32, (cap, LANES), 0)
    for s in range(n_slot):
        want = r.astype(F32) * copies[s:s + 1, :] + my_rank[s:s + 1, :]
        trk[s * cap:(s + 1) * cap, :] = want
    o_odd[...] = jnp.zeros_like(o_odd)

    def clear(q, carry):
        acc[q] = jnp.zeros(acc.shape[1:], F32)
        return carry

    lax.fori_loop(0, acc.shape[0], clear, 0)
    stage_near(0)
    start_near(AHEAD)
    hand_meta(idx_all, 0)
    wait_meta(idx_all, 0)
    earlier = (lax.broadcasted_iota(jnp.int32, (n_tok, n_tok), 0)
               < lax.broadcasted_iota(jnp.int32, (n_tok, n_tok), 1)).astype(F32).astype(BF16)
    rows_pad = round_up(rows_src, LANES)

    def hits(rank):
        for s in range(n_slot):
            yield s * cap, cap, rank[s:s + 1, :] == trk[s * cap:(s + 1) * cap, 0:1]
        for n in range(odd):
            yield rows_main + n * rows_s, rows_s, rank == float(cap + n) * copies + my_rank

    def route(j, carry):
        idx = idx_all[j].astype(F32)
        has = jnp.zeros((rows_s, n_tok), F32)
        for q in range(n_top):
            has = jnp.where(idx[q:q + 1, :] == e_col, 1.0, has)
        rank = jnp.where(has > 0.0, dot(has.astype(BF16), earlier), -1.0)
        rank_all[j] = rank
        for first, n, hit in hits(rank):
            g_buf[j, first:first + n, :] = jnp.where(hit, 1.0, 0.0).astype(BF16)
        return carry

    def route_gates(j):
        idx = idx_all[j].astype(F32)
        gates = gate_all[j]
        gate = jnp.zeros((rows_s, n_tok), F32)
        for q in range(n_top):
            gate = jnp.where(idx[q:q + 1, :] == e_col, gates[q:q + 1, :], gate)
        parts = []
        for first, n, hit in hits(rank_all[j]):
            s = first // cap
            parts.append(jnp.where(hit, gate[s:s + 1, :] if first < rows_main else gate, 0.0))
        if rows_pad > rows_src:
            parts.append(jnp.zeros((rows_pad - rows_src, n_tok), F32))
        left_over = jnp.transpose(jnp.concatenate(parts, axis=0))[:, :rows_src]
        for n in range(3):
            term = left_over.astype(BF16)
            c_buf[j, n * n_tok:(n + 1) * n_tok, :] = term
            left_over = left_over - term.astype(F32)

    lax.fori_loop(0, n_dev, route, 0)
    stage_near(1)
    start_near(AHEAD + 1)
    send_meta(gate_all, 1)
    route_gates(0)
    stage_far(0)

    chunks = [(n, min(2 * LANES, d_ff - n)) for n in range(0, d_ff, 2 * LANES)]
    n_mid = d_ff // LANES

    def up_block(kb, last, after):
        arrived(xall.at[pl.ds(0, CHIPS), kb], sib_rs.at[kb])

        for j in range(n_dev):
            rows = dot(g_buf[j], xall[j, kb])
            main = rows[:rows_main].astype(BF16)
            for s in range(n_slot):
                xg[s, j * cap:(j + 1) * cap, :] = main[s * cap:(s + 1) * cap]
            for n in range(odd):
                first = rows_main + n * rows_s
                for h in range(kb_w // LANES):
                    xg_odd[n, h, pl.ds(j, rows_s, stride=n_dev), :] = rows[first:first + rows_s, h * LANES:(h + 1) * LANES]
        for n in range(odd):
            for h in range(kb_w // LANES):
                for s in range(n_slot):
                    xg[s, d_main + n * n_dev:d_main + (n + 1) * n_dev, h * LANES:(h + 1) * LANES] = (
                        xg_odd[n, h, s * n_dev:(s + 1) * n_dev, :].astype(BF16))
        for g, (s0, n_s) in enumerate(groups):
            up_load(kb, g).wait()
            for s in range(s0, s0 + n_s):
                for n0, nw in chunks:
                    v = dot(xg[s], wu[s, :, n0:n0 + nw])
                    for n in range(0, nw, LANES):
                        q = s * n_mid + (n0 + n) // LANES
                        part = acc[q, :d_mid, :] + v[:, n:n + LANES]
                        if last:
                            h_buf[s, :, n0 + n:n0 + n + LANES] = gelu(part).astype(BF16)
                        else:
                            acc[q, :d_mid, :] = part
            if not last:
                up_load(kb + 1, g).start()
            if g in after:
                after[g]()

    def up_step(kb, carry):
        def near_2():
            @pl.when(kb + 2 < n_kb)
            def _():
                stage_near(kb + 2)

            @pl.when(kb + 2 + AHEAD < n_kb)
            def _():
                start_near(kb + 2 + AHEAD)

        def gates():
            @pl.when(kb == 1)
            def _():
                hand_meta(gate_all, 1)

            @pl.when(kb == 2)
            def _():
                wait_meta(gate_all, 1)

            @pl.when((kb >= 2) & (kb < 2 + n_dev // 2))
            def _():
                route_gates(2 * (kb - 2) + 1)
                route_gates(jnp.minimum(2 * (kb - 2) + 2, n_dev - 1))

        up_block(kb, False, {0: near_2, 1: lambda: stage_far(kb + 1), 2: gates})
        return carry

    assert n_kb - 1 >= 2 + n_dev // 2
    lax.fori_loop(0, n_kb - 1, up_step, 0)
    up_block(n_kb - 1, True, {})

    def mine(cb, off, h):
        return (cb * CHIPS + off) * 2 + h

    def staged(cb, off, h):
        return n_cb * CHIPS * 2 + ((cb % STAGES) * CHIPS + off) * 2 + h

    tok = pl.ds(0, n_tok)

    lots = {2: 0, 1: 1, prev: 1, 0: 2}

    def to_sib(cb, off):
        return rcopy(acc.at[pl.ds(staged(cb, off, 0), 2), tok], sib_in.at[cb, off], ps_ss.at[cb % STAGES], ps_rs.at[cb % 2, lots[off]], sib)

    def to_far(cb):
        return (rcopy(acc.at[mine(cb, 2, 0), tok], far_in.at[cb, 0], out_ss.at[3], pf_rs.at[cb], right),
                rcopy(acc.at[mine(cb, 2, 1), tok], far_in.at[cb, 1], out_ss.at[3], pf_rs.at[cb], left))

    def to_dir(cb):
        return (rcopy(acc.at[mine(cb, 1, 1), tok], sum_in.at[cb, 2], out_ss.at[4], fin_rs.at[cb], right),
                rcopy(acc.at[mine(cb, prev, 0), tok], sum_in.at[cb, 3], out_ss.at[4], fin_rs.at[cb], left))

    def to_mrg(cb):
        return (rcopy(far_in.at[cb, 0], sum_in.at[cb, 0], out_ss.at[5], fin_rs.at[cb], right),
                rcopy(far_in.at[cb, 1], sum_in.at[cb, 1], out_ss.at[5], fin_rs.at[cb], left))

    def merge(cb):
        arrived(far_in.at[cb], pf_rs.at[cb])
        for h, off in ((0, 1), (1, prev)):
            far_in[cb, h] = far_in[cb, h] + acc[mine(cb, off, h), :n_tok, :]
            to_mrg(cb)[h].start()

    def y_copy(cb):
        columns = pl.ds(pl.multiple_of(cb * cb_w, cb_w), cb_w)
        return pltpu.make_async_copy(y_buf.at[cb], y_ref.at[:, columns], y_s.at[cb])

    def finish(cb):
        arrived(sum_in.at[cb], fin_rs.at[cb])
        for h in range(2):
            out = acc[mine(cb, 0, h), :n_tok, :] + sum_in[cb, h] + sum_in[cb, 3 - h]
            y_buf[cb, :, h * LANES:(h + 1) * LANES] = out
        y_copy(cb).start()

    def add_sib(cb, off):
        for h in range(2):
            q = mine(cb, off, h)
            acc[q, :n_tok, :] = acc[q, :n_tok, :] + sib_in[cb, off, h]

    def combine(j, q):
        v = dot(c_buf[j], o_buf[j])
        v = (v[2 * n_tok:] + v[n_tok:2 * n_tok]) + v[:n_tok]
        for h in range(2):
            acc[q + h, :n_tok, :] = v[:, h * LANES:(h + 1) * LANES]

    def down_step(cb, carry):
        for g in range(len(groups)):
            down_load(cb, g).wait()
        for g, (s0, n_s) in enumerate(groups):
            for s in range(s0, s0 + n_s):
                out = dot(h_buf[s], wd[s])
                main = out[:d_main].astype(BF16)
                for j in range(n_dev):
                    o_buf[j, s * cap:(s + 1) * cap, :] = main[j * cap:(j + 1) * cap]
                for n in range(odd):
                    first = d_main + n * n_dev
                    for h in range(cb_w // LANES):
                        o_odd[n, h, pl.ds(s, n_dev, stride=rows_s), :] = out[first:first + n_dev, h * LANES:(h + 1) * LANES]


        for n in range(odd):
            first = rows_main + n * rows_s
            for h in range(cb_w // LANES):
                for j in range(n_dev):
                    o_buf[j, first:first + rows_s, h * LANES:(h + 1) * LANES] = o_odd[n, h, j * rows_s:(j + 1) * rows_s, :].astype(BF16)

        @pl.when(cb >= STAGES)
        def _():
            took(acc.at[pl.ds(staged(cb, 0, 0), 2 * CHIPS), tok], ps_ss.at[cb % STAGES])

        @pl.when(cb + 1 < n_cb)
        def _():
            for g in range(len(groups)):
                down_load(cb + 1, g).start()

        @pl.when(cb == 1)
        def _():
            merge(cb - 1)

        def for_sib(off):
            combine(2 * off + 1, staged(cb, off, 0))
            to_sib(cb, off).start()

        for off in (2, 1, prev):
            for_sib(off)
        combine(2 * 2, mine(cb, 2, 0))
        arrived(sib_in.at[cb, 2], ps_rs.at[cb % 2, 0])
        add_sib(cb, 2)
        for c in to_far(cb):
            c.start()
        for_sib(0)
        for off in (1, prev):
            combine(2 * off, mine(cb, off, 0))
        arrived(sib_in.at[cb, pl.ds(0, 2)], ps_rs.at[cb % 2, 1])
        for n, off in enumerate((1, prev)):
            add_sib(cb, off)
            to_dir(cb)[n].start()
        combine(0, mine(cb, 0, 0))

        @pl.when(cb >= LAG)
        def _():
            finish(cb - LAG)

        arrived(sib_in.at[cb, 0], ps_rs.at[cb % 2, 2])
        add_sib(cb, 0)

        @pl.when(cb >= 2)
        def _():
            merge(cb - 1)
        return carry

    lax.fori_loop(0, n_cb, down_step, 0)
    merge(n_cb - 1)
    for cb in range(max(0, n_cb - LAG), n_cb):
        finish(cb)

    others = pl.ds(1, n_dev - 1)
    took(idx_all.at[others], meta_ss.at[0])
    took(gate_all.at[others], meta_ss.at[1])
    for n, ref in enumerate((xall.at[pl.ds(0, 2)], xall.at[4], xall.at[pl.ds(0, CHIPS)], far_in, far_in, far_in)):
        took(ref, out_ss.at[n])
    for n in range(min(STAGES, n_cb)):
        took(acc.at[pl.ds(staged(n, 0, 0), 2 * CHIPS), tok], ps_ss.at[n])
    for cb in range(n_cb):
        y_copy(cb).wait()


def solution(mesh):
    assert mesh.shape["ep"] == 2 * CHIPS

    def group_layer(tokens, topk_idx, topk_w, w_up, w_down, slot_expert):
        n_tok, d_model = tokens.shape
        n_top = topk_idx.shape[1]
        n_dev, n_slot = slot_expert.shape
        d_ff = w_up.shape[-1]
        bound = slot_bound(n_tok, n_top, n_dev, n_slot)
        cap = bound // 8 * 8
        odd, rows_s = bound - cap, round_up(n_slot, 16)
        kb_w, cb_w = 2 * LANES, 2 * LANES
        n_kb, n_cb = d_model // kb_w, d_model // cb_w
        d_mid = n_dev * bound
        rows_src = n_slot * cap + odd * rows_s
        n_acc = max(n_slot * (d_ff // LANES), (n_cb + STAGES) * CHIPS * 2)
        cfg = dict(bound=bound, cap=cap, kb_w=kb_w, cb_w=cb_w)
        dma = pltpu.SemaphoreType.DMA
        hbm = pl.BlockSpec(memory_space=pl.ANY)
        return pl.pallas_call(
            functools.partial(moe_kernel, cfg),
            out_shape=jax.ShapeDtypeStruct((n_tok, d_model), F32),
            in_specs=[hbm] * 6,
            out_specs=hbm,
            scratch_shapes=[
                pltpu.VMEM((n_dev, n_kb, n_tok, kb_w), BF16),
                pltpu.VMEM((n_dev, n_top, n_tok), jnp.int32),
                pltpu.VMEM((n_dev, n_top, n_tok), F32),
                pltpu.VMEM((n_dev, rows_s, n_tok), F32),
                pltpu.VMEM((n_dev, n_slot), jnp.int32),
                pltpu.VMEM((n_slot * cap, LANES), F32),
                pltpu.VMEM((n_dev, rows_src, n_tok), BF16),
                pltpu.VMEM((n_dev, 3 * n_tok, rows_src), BF16),
                pltpu.VMEM((n_slot, d_mid, kb_w), BF16),
                pltpu.VMEM((odd, kb_w // LANES, rows_s * n_dev, LANES), F32),
                pltpu.VMEM((n_acc, max(d_mid, n_tok), LANES), F32),
                pltpu.VMEM((n_slot, d_mid, d_ff), BF16),
                pltpu.VMEM((n_dev, rows_src, cb_w), BF16),
                pltpu.VMEM((odd, cb_w // LANES, n_dev * rows_s, LANES), F32),
                pltpu.VMEM((n_slot, kb_w, d_ff), BF16),
                pltpu.VMEM((n_slot, d_ff, cb_w), BF16),
                pltpu.VMEM((n_cb, CHIPS, 2, n_tok, LANES), F32),
                pltpu.VMEM((n_cb, 2, n_tok, LANES), F32),
                pltpu.VMEM((n_cb, 4, n_tok, LANES), F32),
                pltpu.VMEM((n_cb, n_tok, cb_w), F32),
                dma((4,)), dma((2,)), dma((2, 2)), dma((6,)),
                dma((n_kb,)), dma((n_kb,)), dma((n_kb,)),
                dma((-(-n_slot // GROUP),)), dma((-(-n_slot // GROUP),)),
                dma((STAGES,)), dma((2, 3)), dma((n_cb,)), dma((n_cb,)), dma((n_cb,)),
            ],
            compiler_params=pltpu.CompilerParams(collective_id=0, has_side_effects=True, vmem_limit_bytes=67_000_000),
        )(tokens, topk_idx.T, topk_w.T, slot_expert, w_up, w_down).astype(BF16)

    row_spec = P(('dp', 'ep'), None)
    weight_spec = P('ep', None, None, None)
    return jax.shard_map(group_layer, mesh=mesh, in_specs=(row_spec, row_spec, row_spec, weight_spec, weight_spec, P(None, None)),
                         out_specs=row_spec, check_vma=False)
```
